32 devices in a mesh: tm: 32 (over z, y, x, core), chan: 1.
Axes of the slice: x: 2, y: 2, z: 4, core: 2. Of those that a mesh axis runs over, the one named last changes fastest.
Arguments:
- signal: bfloat16 [3, 4096, 512], P(None, 'tm', 'chan'), may hold values from -6 to 6
- taps: float32 [10, 2, 512], P(None, None, 'chan'), may hold values from -3 to 3
- w_gate: bfloat16 [10, 512, 2, 512], P(None, None, None, 'chan'), may hold values from -0.25 to 0.25
- w_res: bfloat16 [10, 512, 512], P(None, None, 'chan'), may hold values from -0.25 to 0.25
- w_skip: bfloat16 [10, 512, 512], P(None, None, 'chan'), may hold values from -0.1875 to 0.1875
Outputs:
- stream: bfloat16 [3, 4096, 512], P(None, 'tm', 'chan')
- skips: bfloat16 [3, 4096, 512], P(None, 'tm', 'chan')
The draws below stay inside these ranges and needn't reach their ends.
All inputs are finite; a program needn't handle non-finite values.
Results may differ from the reference program's by a relative error of at most 0.02.
Values may be sent and summed in bfloat16 or wider, within the bound.
A program may use at most 64 MiB of HBM per device.

```python
import jax
import jax.numpy as jnp

C = 512
LAYERS = 10
SEQS = 3
LEN = 4096


def level_of(rng, extent, pieces, low, high):
    gain, own = 1.0, jax.random.fold_in(rng, 6)
    for dim, parts in pieces:
        draws = jnp.exp(jax.random.uniform(jax.random.fold_in(own, dim), (parts,), jnp.float32, low / len(pieces), high / len(pieces)))
        gain = gain * jnp.repeat(draws, extent[dim] // parts).reshape([-1 if axis == dim else 1 for axis in range(len(extent))])
    return gain


def noise(rng, dims, deviation, most, pieces=(), held_as=jnp.bfloat16):
    drawn = jax.random.normal(rng, dims, jnp.float32) * deviation
    if len(pieces) > 0:
        drawn = level_of(rng, dims, pieces, -0.22, 0.18) * drawn
    return jnp.clip(drawn, min=-most, max=most).astype(held_as)


def setup_inputs(seed: int = 0) -> dict:
    streams_of = jax.random.split(jax.random.key(seed), 6)
    signal = noise(streams_of[0], (SEQS, LEN, C), 1.0, 6.0, ((1, 32),))
    taps = noise(streams_of[1], (LAYERS, 2, C), 0.8, 3.0, (), jnp.float32)
    w_gate = noise(streams_of[2], (LAYERS, C, 2, C), C ** -0.5, 0.25)
    w_res = noise(streams_of[3], (LAYERS, C, C), C ** -0.5, 0.25)
    w_skip = noise(streams_of[4], (LAYERS, C, C), (C * 2) ** -0.5, 0.1875)
    return {"signal": signal, "taps": taps, "w_gate": w_gate, "w_res": w_res, "w_skip": w_skip}


def reference(signal, taps, w_gate, w_res, w_skip):
    stream = signal
    skip = jnp.zeros((SEQS, LEN, C), jnp.float32)
    for layer in range(LAYERS):
        delay = 2 ** layer
        delayed = jnp.concatenate([jnp.zeros((SEQS, delay, C), jnp.bfloat16), stream[:, :LEN - delay]], axis=1)
        conv = (taps[layer, 0] * delayed.astype(jnp.float32) + taps[layer, 1] * stream.astype(jnp.float32)).astype(jnp.bfloat16)
        hidden = jnp.einsum("stc,cko->stko", conv.astype(jnp.float32), w_gate[layer].astype(jnp.float32))
        gated = (jnp.tanh(hidden[:, :, 0]) * jax.nn.sigmoid(hidden[:, :, 1])).astype(jnp.bfloat16)
        gated_f = gated.astype(jnp.float32)
        stream = (stream.astype(jnp.float32) + jnp.einsum("stc,co->sto", gated_f, w_res[layer].astype(jnp.float32))).astype(jnp.bfloat16)
        skip = skip + jnp.einsum("stc,co->sto", gated_f, w_skip[layer].astype(jnp.float32))
    return stream, skip.astype(jnp.bfloat16)
```

```python
import functools

import jax
import jax.numpy as jnp
from jax import lax
from jax.experimental import pallas as pl
from jax.experimental.pallas import tpu as pltpu
from jax.sharding import PartitionSpec as P

MESH = pl.DeviceIdType.MESH
BF16, F32 = jnp.bfloat16, jnp.float32
ALIGN = 16
VMEM_LIMIT = 56000 * 1024


def shifted(value, axis, steps):
    count = lax.axis_size(axis)
    leading, last = (max(0, -steps), min(count, count - steps))
    return lax.ppermute(value, axis, [(source, source + steps) for source in range(leading, last)])


def delay_block(stream, delay, near_fn, far_fn):
    length = stream.shape[1]
    whole, rest = divmod(delay, length)
    if whole == 0:
        nearer = stream
    else:
        nearer = near_fn(stream, whole)
    if rest == 0:
        return nearer
    farther = far_fn(stream[:, length - rest :], whole + 1)
    return jnp.concatenate([farther, nearer[:, : length - rest]], axis=1)


def near_time(block, steps):
    return shifted(block, "tm", steps)


def far_time(block, steps):
    return shifted(block, "tm", steps)


def gate_units(hidden):
    return (jnp.tanh(hidden[:, :, 0]) * jax.nn.sigmoid(hidden[:, :, 1])).astype(jnp.bfloat16)


def local(signal, taps, w_gate, w_res, w_skip):
    stream = signal
    seqs, length, local_c = stream.shape
    skip = jnp.zeros((seqs, length, local_c), jnp.float32)
    for layer in range(taps.shape[0]):
        delayed = delay_block(stream, 2**layer, near_time, far_time)
        conv = (
            taps[layer, 0] * delayed.astype(jnp.float32)
            + taps[layer, 1] * stream.astype(jnp.float32)
        ).astype(jnp.bfloat16)
        gate_w = w_gate[layer]
        hidden = jnp.einsum(
            "stc,cko->stko",
            lax.all_gather(conv, "chan", axis=2, tiled=True),
            gate_w,
            preferred_element_type=jnp.float32,
        )
        gated = gate_units(hidden)
        res_w = w_res[layer]
        skip_w = w_skip[layer]
        piece = lax.all_gather(gated, "chan", axis=2, tiled=True)
        update = jnp.einsum("stc,co->sto", piece, res_w, preferred_element_type=jnp.float32)
        skip_part = jnp.einsum("stc,co->sto", piece, skip_w, preferred_element_type=jnp.float32)
        stream = (stream.astype(jnp.float32) + update).astype(jnp.bfloat16)
        skip = skip + skip_part
    return (stream, skip.astype(jnp.bfloat16))


def tanh_gate(filt, gate):
    return (jnp.tanh(filt) * (0.5 * jnp.tanh(0.5 * gate) + 0.5)).astype(BF16)


def split_pairs(pairs, out):
    width = pairs.shape[0]
    block = min(128, width)
    row = lax.broadcasted_iota(jnp.int32, (2 * block, 2 * block), 0)
    column = lax.broadcasted_iota(jnp.int32, (2 * block, 2 * block), 1)
    wanted = jnp.where(row < block, 2 * row, 2 * (row - block) + 1)
    order = jnp.where(column == wanted, 1.0, 0.0).astype(F32).astype(BF16)
    for at in range(0, width, block):
        both = pairs[at : at + block].reshape(2 * block, pairs.shape[2])
        sorted_rows = jnp.dot(order, both, preferred_element_type=F32).astype(BF16)
        out[0, at : at + block] = sorted_rows[:block]
        out[1, at : at + block] = sorted_rows[block:]


P1, P2, P3, P4, P9 = range(5)
REACH = 4


def kernel(n, layers, near, sig_hbm, taps_hbm, wg_hbm, wr_hbm, ws_hbm, out_x, out_skip, *scratch):
    sig, taps, raw, wg, wr, ws, xs, zs, skip, ahead, far = scratch[:11]
    in_sem, w_sem, send_sem, recv_sem, far_send, far_recv = scratch[11:17]
    halos = scratch[17:]
    seqs, length, width = sig.shape
    me = lax.axis_index("tm")
    place = lax.rem(me, 4)
    core = lax.rem(me, 2)
    clean = near - 1
    rows_of = [max(ALIGN, 2**layer) for layer in range(near)]
    half = min(256, width)
    every = list(range(seqs))

    def weights(layer):
        return [
            pltpu.make_async_copy(wg_hbm.at[layer], raw.at[layer], w_sem.at[layer, 0]),
            pltpu.make_async_copy(wr_hbm.at[layer], wr.at[layer], w_sem.at[layer, 1]),
            pltpu.make_async_copy(ws_hbm.at[layer], ws.at[layer], w_sem.at[layer, 2]),
        ]

    inputs = [
        pltpu.make_async_copy(sig_hbm, sig, in_sem.at[0]),
        pltpu.make_async_copy(taps_hbm, taps, in_sem.at[1]),
    ]
    for copy in inputs:
        copy.start()
    for layer in range(layers):
        for copy in weights(layer):
            copy.start()

    barrier = pltpu.get_barrier_semaphore()
    for step in range(1, REACH + 1):
        for ok, other in ((me + step < n, me + step), (me >= step, me - step)):

            @pl.when(ok)
            def _(other=other):
                pl.semaphore_signal(barrier, inc=1, device_id={"tm": other}, device_id_type=MESH)

    def source(layer):
        return sig if layer == 0 else xs.at[layer - 1]

    def send(layer, s):
        rows = rows_of[layer]
        return pltpu.make_async_remote_copy(
            src_ref=source(layer).at[s, pl.ds(length - rows, rows)],
            dst_ref=halos[layer].at[s],
            send_sem=send_sem.at[layer, s],
            recv_sem=recv_sem.at[layer, s],
            device_id={"tm": me + 1},
            device_id_type=MESH,
        )

    def start_send(layer):
        @pl.when(me + 1 < n)
        def _():
            for s in every:
                send(layer, s).start()

    def take(layer):
        @pl.when(me >= 1)
        def _():
            for s in every:
                send(layer, s).wait_recv()

        @pl.when(me < 1)
        def _():
            for s in every:
                halos[layer][s] = jnp.zeros(halos[layer].shape[1:], BF16)

    def ship(slot, s, block, where, other):
        return pltpu.make_async_remote_copy(
            src_ref=block.at[s],
            dst_ref=far.at[where, s],
            send_sem=far_send.at[slot, s],
            recv_sem=far_recv.at[where, s],
            device_id={"tm": other},
            device_id_type=MESH,
        )

    last_near, last_far = xs.at[near - 1], xs.at[layers - 2]
    relay = (place == 3) & (me >= 7)
    routes = {
        "own": [
            ((place == 3) & (me + 4 < n), 0, last_near, P4, me + 4),
            ((place != 3) & (me + 2 < n), 0, last_near, P2, me + 2),
            ((place == 1) & (me + 3 < n), 1, last_near, P3, me + 3),
            (core == 0, 1, last_near, P1, me + 1),
        ],
        "relay": [
            (relay, 2, far.at[P4], P2, me - 2),
            (relay, 3, far.at[P4], P3, me - 1),
        ],
        "share": [
            ((core == 1) & (me >= 2), 4, far.at[P2], P1, me - 1),
            ((core == 0) & (me >= 2), 4, far.at[P2], P3, me + 1),
        ],
        "last": [(me + 4 < n, 5, last_far, P9, me + 4)],
    }

    def go(kind, s):
        for ok, slot, block, where, other in routes[kind]:

            @pl.when(ok)
            def _(slot=slot, block=block, where=where, other=other):
                ship(slot, s, block, where, other).start()

    def get(where, s, least):
        @pl.when(me >= least)
        def _():
            ship(0, s, last_near, where, me).wait_recv()

        @pl.when(me < least)
        def _():
            far[where, s] = jnp.zeros(far.shape[2:], BF16)

    def load(layer, s, low, high):
        return source(layer)[s, low:high]

    def stack(parts):
        return jnp.concatenate(parts, axis=0) if len(parts) > 1 else parts[0]

    def gated(layer, late, own_f):
        conv = (taps[layer, 0:1] * late.astype(F32) + taps[layer, 1:2] * own_f).astype(BF16)
        parts = []
        for at in range(0, width, half):
            filt = jnp.dot(conv, wg[layer, 0, :, at : at + half], preferred_element_type=F32)
            gate = jnp.dot(conv, wg[layer, 1, :, at : at + half], preferred_element_type=F32)
            parts.append(tanh_gate(filt, gate))
        return jnp.concatenate(parts, axis=1) if len(parts) > 1 else parts[0]

    def columns():
        return [slice(at, at + half) for at in range(0, width, half)]

    def renewed(layer, z, own_f, cols):
        return (own_f[:, cols] + jnp.dot(z, wr[layer, :, cols], preferred_element_type=F32)).astype(BF16)

    def finish(layer, delayed, own, which, low, high):
        count = high - low
        own_f = stack(own).astype(F32)
        z = gated(layer, stack(delayed), own_f)
        for i, s in enumerate(which):
            zs[layer, s, low:high] = z[i * count : (i + 1) * count]
        for cols in columns():
            new = renewed(layer, z, own_f, cols)
            for i, s in enumerate(which):
                xs[layer, s, low:high, cols] = new[i * count : (i + 1) * count]

    top = [max(ALIGN, 2 ** (layer + 1)) for layer in range(clean)]
    first = [0] * clean
    for layer in range(clean - 1, -1, -1):
        need = top[layer] if layer == clean - 1 else first[layer + 1] - 2 ** (layer + 1)
        first[layer] = max(0, min(need, top[layer]) // ALIGN * ALIGN)

    def arrive(layer):
        for copy in weights(layer):
            copy.wait()
        split_pairs(raw.at[layer], wg.at[layer])

    for copy in inputs:
        copy.wait()
    for layer in range(clean):
        delay, low = 2**layer, first[layer]
        arrive(layer)
        delayed, own = [], []
        for s in every:
            if delay < ALIGN:
                begin = max(0, low - ALIGN)
                block = pltpu.roll(load(layer, s, begin, length).astype(F32), delay, 0)
                delayed.append(block[low - begin :])
            else:
                delayed.append(load(layer, s, low - delay, length - delay))
            own.append(load(layer, s, low, length))
        finish(layer, delayed, own, every, low, length)
        if layer == 0:
            total = sum(
                ((me + step < n).astype(jnp.int32) + (me >= step).astype(jnp.int32)) for step in range(1, REACH + 1)
            )
            pl.semaphore_wait(barrier, total)
            start_send(0)
        start_send(layer + 1)

    arrive(clean)

    for layer in range(clean):
        delay, high = 2**layer, top[layer]
        take(layer)
        delayed, own = [], []
        for s in every:
            rows = rows_of[layer]
            tail = halos[layer][s]
            if delay < ALIGN:
                joined = jnp.concatenate([tail.astype(F32), load(layer, s, 0, high).astype(F32)], axis=0)
                delayed.append(pltpu.roll(joined, delay, 0)[rows:])
            else:
                delayed.append(jnp.concatenate([tail, load(layer, s, 0, high - delay)], axis=0))
            own.append(load(layer, s, 0, high))
        finish(layer, delayed, own, every, 0, high)

    take(clean)
    for s in every:
        late = jnp.concatenate([halos[clean][s], load(clean, s, 0, length - 2**clean)], axis=0)
        finish(clean, [late], [load(clean, s, 0, length)], [s], 0, length)
        go("own", s)

    for layer in range(near, layers):
        arrive(layer)

    def held_skip(span):
        for cols in columns():
            total = None
            for before in span:
                z = zs[before].reshape(seqs * length, width)
                more = jnp.dot(z, ws[before, :, cols], preferred_element_type=F32)
                total = more if total is None else total + more
            total = total.reshape(seqs, length, half)
            skip[:, :, cols] = total if span[0] == 0 else skip[:, :, cols] + total

    held_skip(range(near))

    for s in every:

        @pl.when(relay)
        def _(s=s):
            ship(0, s, last_near, P4, me).wait_recv()

        go("relay", s)
        get(P2, s, 2)
        go("share", s)
        get(P1, s, 1)
        get(P3, s, 3)
        late = jnp.concatenate([far[P1, s], far[P3, s]], axis=0)
        own_f = jnp.concatenate([xs[near - 1, s], far[P2, s]], axis=0).astype(F32)
        z = gated(near, late, own_f)
        zs[near, s] = z[:length]
        for cols in columns():
            new = renewed(near, z, own_f, cols)
            xs[near, s, :, cols] = new[:length]
            ahead[s, :, cols] = new[length:]
        own_f = xs[near, s].astype(F32)
        z = gated(near + 1, ahead[s], own_f)
        zs[near + 1, s] = z
        for cols in columns():
            xs[near + 1, s, :, cols] = renewed(near + 1, z, own_f, cols)
        go("last", s)

    held_skip(range(near, layers - 1))

    final = layers - 1
    for s in every:
        get(P9, s, 4)
        own_f = xs[final - 1, s].astype(F32)
        z = gated(final, far[P9, s], own_f)
        for cols in columns():
            out_x[s, :, cols] = renewed(final, z, own_f, cols)
        for cols in columns():
            more = jnp.dot(z, ws[final, :, cols], preferred_element_type=F32)
            out_skip[s, :, cols] = (skip[s, :, cols] + more).astype(BF16)

    @pl.when(me + 1 < n)
    def _():
        for layer in range(near):
            for s in every:
                send(layer, s).wait_send()

    for route in routes.values():
        for ok, slot, block, where, other in route:

            @pl.when(ok)
            def _(slot=slot, block=block, where=where, other=other):
                for s in every:
                    ship(slot, s, block, where, other).wait_send()


def fused(n, signal, taps, w_gate, w_res, w_skip):
    seqs, length, width = signal.shape
    layers = taps.shape[0]
    near = length.bit_length() - 1
    halos = [pltpu.VMEM((seqs, max(ALIGN, 2**layer), width), BF16) for layer in range(near)]
    flops = 2 * seqs * length * width * width * 4 * layers
    in_vmem, anywhere = pl.BlockSpec(memory_space=pltpu.VMEM), pl.BlockSpec(memory_space=pl.ANY)
    return pl.pallas_call(
        functools.partial(kernel, n, layers, near),
        out_shape=[pltpu.VMEM(signal.shape, BF16)] * 2,
        in_specs=[anywhere] * 5,
        out_specs=[in_vmem, in_vmem],
        scratch_shapes=[
            pltpu.VMEM(signal.shape, BF16),
            pltpu.VMEM(taps.shape, F32),
            pltpu.VMEM((layers, width, 2, width), BF16),
            pltpu.VMEM((layers, 2, width, width), BF16),
            pltpu.VMEM((layers, width, width), BF16),
            pltpu.VMEM((layers, width, width), BF16),
            pltpu.VMEM((layers - 1, seqs, length, width), BF16),
            pltpu.VMEM((layers - 1, seqs, length, width), BF16),
            pltpu.VMEM((seqs, length, width), F32),
            pltpu.VMEM((seqs, length, width), BF16),
            pltpu.VMEM((5, seqs, length, width), BF16),
            pltpu.SemaphoreType.DMA((2,)),
            pltpu.SemaphoreType.DMA((layers, 3)),
            pltpu.SemaphoreType.DMA((near, seqs)),
            pltpu.SemaphoreType.DMA((near, seqs)),
            pltpu.SemaphoreType.DMA((6, seqs)),
            pltpu.SemaphoreType.DMA((5, seqs)),
            *halos,
        ],
        compiler_params=pltpu.CompilerParams(collective_id=0, has_side_effects=True, vmem_limit_bytes=VMEM_LIMIT),
        cost_estimate=pl.CostEstimate(flops=flops, bytes_accessed=8 * layers * width * width, transcendentals=0),
        name="stack",
    )(signal, taps, w_gate, w_res, w_skip)


def solution(mesh):
    in_specs = (
        P(None, "tm", "chan"),
        P(None, None, "chan"),
        P(None, None, None, "chan"),
        P(None, None, "chan"),
        P(None, None, "chan"),
    )
    out_specs = (P(None, "tm", "chan"), P(None, "tm", "chan"))

    def body(*args):
        n, length, layers = mesh.shape["tm"], args[0].shape[1], args[1].shape[0]
        fits = length >= 4 * ALIGN and 2 ** (layers - 3) == length and n % 4 == 0
        if mesh.shape["chan"] == 1 and fits:
            return tuple(fused(n, *args))
        return local(*args)

    return jax.shard_map(body, mesh=mesh, in_specs=in_specs, out_specs=out_specs, check_vma=False)
```

```python
import functools

import jax
import jax.numpy as jnp
from jax import lax
from jax.experimental import pallas as pl
from jax.experimental.pallas import tpu as pltpu
from jax.sharding import PartitionSpec as P

MESH = pl.DeviceIdType.MESH
BF16, F32 = jnp.bfloat16, jnp.float32
ALIGN = 16
VMEM_LIMIT = 56000 * 1024


def shifted(value, axis, steps):
    count = lax.axis_size(axis)
    leading, last = (max(0, -steps), min(count, count - steps))
    return lax.ppermute(value, axis, [(source, source + steps) for source in range(leading, last)])


def delay_block(stream, delay, near_fn, far_fn):
    length = stream.shape[1]
    whole, rest = divmod(delay, length)
    if whole == 0:
        nearer = stream
    else:
        nearer = near_fn(stream, whole)
    if rest == 0:
        return nearer
    farther = far_fn(stream[:, length - rest :], whole + 1)
    return jnp.concatenate([farther, nearer[:, : length - rest]], axis=1)


def near_time(block, steps):
    return shifted(block, "tm", steps)


def far_time(block, steps):
    return shifted(block, "tm", steps)


def gate_units(hidden):
    return (jnp.tanh(hidden[:, :, 0]) * jax.nn.sigmoid(hidden[:, :, 1])).astype(jnp.bfloat16)


def local(signal, taps, w_gate, w_res, w_skip):
    stream = signal
    seqs, length, local_c = stream.shape
    skip = jnp.zeros((seqs, length, local_c), jnp.float32)
    for layer in range(taps.shape[0]):
        delayed = delay_block(stream, 2**layer, near_time, far_time)
        conv = (
            taps[layer, 0] * delayed.astype(jnp.float32)
            + taps[layer, 1] * stream.astype(jnp.float32)
        ).astype(jnp.bfloat16)
        gate_w = w_gate[layer]
        hidden = jnp.einsum(
            "stc,cko->stko",
            lax.all_gather(conv, "chan", axis=2, tiled=True),
            gate_w,
            preferred_element_type=jnp.float32,
        )
        gated = gate_units(hidden)
        res_w = w_res[layer]
        skip_w = w_skip[layer]
        piece = lax.all_gather(gated, "chan", axis=2, tiled=True)
        update = jnp.einsum("stc,co->sto", piece, res_w, preferred_element_type=jnp.float32)
        skip_part = jnp.einsum("stc,co->sto", piece, skip_w, preferred_element_type=jnp.float32)
        stream = (stream.astype(jnp.float32) + update).astype(jnp.bfloat16)
        skip = skip + skip_part
    return (stream, skip.astype(jnp.bfloat16))


def tanh_gate(filt, gate):
    return (jnp.tanh(filt) * (0.5 * jnp.tanh(0.5 * gate) + 0.5)).astype(BF16)


def split_pairs(pairs, out):
    width = pairs.shape[0]
    block = min(128, width)
    row = lax.broadcasted_iota(jnp.int32, (2 * block, 2 * block), 0)
    column = lax.broadcasted_iota(jnp.int32, (2 * block, 2 * block), 1)
    wanted = jnp.where(row < block, 2 * row, 2 * (row - block) + 1)
    order = jnp.where(column == wanted, 1.0, 0.0).astype(F32).astype(BF16)
    for at in range(0, width, block):
        both = pairs[at : at + block].reshape(2 * block, pairs.shape[2])
        sorted_rows = jnp.dot(order, both, preferred_element_type=F32).astype(BF16)
        out[0, at : at + block] = sorted_rows[:block]
        out[1, at : at + block] = sorted_rows[block:]


P1, P2, P3, P4, P9 = range(5)
REACH = 4


def kernel(n, layers, near, sig_hbm, taps_hbm, wg_hbm, wr_hbm, ws_hbm, out_x, out_skip, *scratch):
    sig, taps, raw, wg, wr, ws, xs, zs, skip, ahead, far = scratch[:11]
    in_sem, w_sem, send_sem, recv_sem, far_send, far_recv, order_sem = scratch[11:18]
    halos = scratch[18:]
    seqs, length, width = sig.shape
    me = lax.axis_index("tm")
    place = lax.rem(me, 4)
    core = lax.rem(me, 2)
    clean = near - 1
    rows_of = [max(ALIGN, 2**layer) for layer in range(near)]
    half = min(256, width)
    every = list(range(seqs))

    def fence():
        pl.semaphore_signal(order_sem, 1)
        pl.semaphore_wait(order_sem, 1)

    def weights(layer):
        return [
            pltpu.make_async_copy(wg_hbm.at[layer], raw.at[layer], w_sem.at[layer, 0]),
            pltpu.make_async_copy(wr_hbm.at[layer], wr.at[layer], w_sem.at[layer, 1]),
            pltpu.make_async_copy(ws_hbm.at[layer], ws.at[layer], w_sem.at[layer, 2]),
        ]

    inputs = [
        pltpu.make_async_copy(sig_hbm, sig, in_sem.at[0]),
        pltpu.make_async_copy(taps_hbm, taps, in_sem.at[1]),
    ]
    for copy in inputs:
        copy.start()
    fence()
    for layer in range(layers):
        for copy in weights(layer):
            copy.start()

    barrier = pltpu.get_barrier_semaphore()
    for step in range(1, REACH + 1):
        for ok, other in ((me + step < n, me + step), (me >= step, me - step)):

            @pl.when(ok)
            def _(other=other):
                pl.semaphore_signal(barrier, inc=1, device_id={"tm": other}, device_id_type=MESH)

    def source(layer):
        return sig if layer == 0 else xs.at[layer - 1]

    def send(layer, s):
        rows = rows_of[layer]
        return pltpu.make_async_remote_copy(
            src_ref=source(layer).at[s, pl.ds(length - rows, rows)],
            dst_ref=halos[layer].at[s],
            send_sem=send_sem.at[layer, s],
            recv_sem=recv_sem.at[layer, s],
            device_id={"tm": me + 1},
            device_id_type=MESH,
        )

    def start_send(layer):
        @pl.when(me + 1 < n)
        def _():
            for s in every:
                send(layer, s).start()

    def take(layer):
        @pl.when(me >= 1)
        def _():
            for s in every:
                send(layer, s).wait_recv()

        @pl.when(me < 1)
        def _():
            for s in every:
                halos[layer][s] = jnp.zeros(halos[layer].shape[1:], BF16)

    def ship(slot, s, block, where, other):
        return pltpu.make_async_remote_copy(
            src_ref=block.at[s],
            dst_ref=far.at[where, s],
            send_sem=far_send.at[slot, s],
            recv_sem=far_recv.at[where, s],
            device_id={"tm": other},
            device_id_type=MESH,
        )

    last_near, last_far = xs.at[near - 1], xs.at[layers - 2]
    relay = (place == 3) & (me >= 7)
    routes = {
        "own": [
            ((place == 3) & (me + 4 < n), 0, last_near, P4, me + 4),
            ((place != 3) & (me + 2 < n), 0, last_near, P2, me + 2),
            ((place == 1) & (me + 3 < n), 1, last_near, P3, me + 3),
            (core == 0, 1, last_near, P1, me + 1),
        ],
        "relay": [
            (relay, 2, far.at[P4], P2, me - 2),
            (relay, 3, far.at[P4], P3, me - 1),
        ],
        "share": [
            ((core == 1) & (me >= 2), 4, far.at[P2], P1, me - 1),
            ((core == 0) & (me >= 2), 4, far.at[P2], P3, me + 1),
        ],
        "last": [(me + 4 < n, 5, last_far, P9, me + 4)],
    }

    def go(kind, s):
        for ok, slot, block, where, other in routes[kind]:

            @pl.when(ok)
            def _(slot=slot, block=block, where=where, other=other):
                ship(slot, s, block, where, other).start()

    def get(where, s, least):
        @pl.when(me >= least)
        def _():
            ship(0, s, last_near, where, me).wait_recv()

        @pl.when(me < least)
        def _():
            far[where, s] = jnp.zeros(far.shape[2:], BF16)

    def load(layer, s, low, high):
        return source(layer)[s, low:high]

    def stack(parts):
        return jnp.concatenate(parts, axis=0) if len(parts) > 1 else parts[0]

    def gated(layer, late, own_f):
        conv = (taps[layer, 0:1] * late.astype(F32) + taps[layer, 1:2] * own_f).astype(BF16)
        parts = []
        for at in range(0, width, half):
            filt = jnp.dot(conv, wg[layer, 0, :, at : at + half], preferred_element_type=F32)
            gate = jnp.dot(conv, wg[layer, 1, :, at : at + half], preferred_element_type=F32)
            parts.append(tanh_gate(filt, gate))
        return jnp.concatenate(parts, axis=1) if len(parts) > 1 else parts[0]

    def columns():
        return [slice(at, at + half) for at in range(0, width, half)]

    def renewed(layer, z, own_f, cols):
        return (own_f[:, cols] + jnp.dot(z, wr[layer, :, cols], preferred_element_type=F32)).astype(BF16)

    def finish(layer, delayed, own, which, low, high):
        count = high - low
        own_f = stack(own).astype(F32)
        z = gated(layer, stack(delayed), own_f)
        for i, s in enumerate(which):
            zs[layer, s, low:high] = z[i * count : (i + 1) * count]
        for cols in columns():
            new = renewed(layer, z, own_f, cols)
            for i, s in enumerate(which):
                xs[layer, s, low:high, cols] = new[i * count : (i + 1) * count]

    top = [max(ALIGN, 2 ** (layer + 1)) for layer in range(clean)]
    first = [0] * clean
    for layer in range(clean - 1, -1, -1):
        need = top[layer] if layer == clean - 1 else first[layer + 1] - 2 ** (layer + 1)
        first[layer] = max(0, min(need, top[layer]) // ALIGN * ALIGN)

    def arrive(layer):
        for copy in weights(layer):
            copy.wait()
        split_pairs(raw.at[layer], wg.at[layer])

    for copy in inputs:
        copy.wait()
    for layer in range(clean):
        delay, low = 2**layer, first[layer]
        arrive(layer)
        delayed, own = [], []
        for s in every:
            if delay < ALIGN:
                begin = max(0, low - ALIGN)
                block = pltpu.roll(load(layer, s, begin, length).astype(F32), delay, 0)
                delayed.append(block[low - begin :])
            else:
                delayed.append(load(layer, s, low - delay, length - delay))
            own.append(load(layer, s, low, length))
        finish(layer, delayed, own, every, low, length)
        if layer == 0:
            total = sum(
                ((me + step < n).astype(jnp.int32) + (me >= step).astype(jnp.int32)) for step in range(1, REACH + 1)
            )
            pl.semaphore_wait(barrier, total)
            start_send(0)
        start_send(layer + 1)

    arrive(clean)

    for layer in range(clean):
        delay, high = 2**layer, top[layer]
        take(layer)
        delayed, own = [], []
        for s in every:
            rows = rows_of[layer]
            tail = halos[layer][s]
            if delay < ALIGN:
                joined = jnp.concatenate([tail.astype(F32), load(layer, s, 0, high).astype(F32)], axis=0)
                delayed.append(pltpu.roll(joined, delay, 0)[rows:])
            else:
                delayed.append(jnp.concatenate([tail, load(layer, s, 0, high - delay)], axis=0))
            own.append(load(layer, s, 0, high))
        finish(layer, delayed, own, every, 0, high)

    take(clean)
    for s in every:
        late = jnp.concatenate([halos[clean][s], load(clean, s, 0, length - 2**clean)], axis=0)
        finish(clean, [late], [load(clean, s, 0, length)], [s], 0, length)
        go("own", s)

    for layer in range(near, layers):
        arrive(layer)

    def held_skip(span):
        for cols in columns():
            total = None
            for before in span:
                z = zs[before].reshape(seqs * length, width)
                more = jnp.dot(z, ws[before, :, cols], preferred_element_type=F32)
                total = more if total is None else total + more
            total = total.reshape(seqs, length, half)
            skip[:, :, cols] = total if span[0] == 0 else skip[:, :, cols] + total

    held_skip(range(near))

    for s in every:

        @pl.when(relay)
        def _(s=s):
            ship(0, s, last_near, P4, me).wait_recv()

        go("relay", s)
        get(P2, s, 2)
        go("share", s)
        get(P1, s, 1)
        get(P3, s, 3)
        late = jnp.concatenate([far[P1, s], far[P3, s]], axis=0)
        own_f = jnp.concatenate([xs[near - 1, s], far[P2, s]], axis=0).astype(F32)
        z = gated(near, late, own_f)
        zs[near, s] = z[:length]
        for cols in columns():
            new = renewed(near, z, own_f, cols)
            xs[near, s, :, cols] = new[:length]
            ahead[s, :, cols] = new[length:]
        own_f = xs[near, s].astype(F32)
        z = gated(near + 1, ahead[s], own_f)
        zs[near + 1, s] = z
        for cols in columns():
            xs[near + 1, s, :, cols] = renewed(near + 1, z, own_f, cols)
        go("last", s)

    held_skip(range(near, layers - 1))

    final = layers - 1
    for s in every:
        get(P9, s, 4)
        own_f = xs[final - 1, s].astype(F32)
        z = gated(final, far[P9, s], own_f)
        for cols in columns():
            out_x[s, :, cols] = renewed(final, z, own_f, cols)
        for cols in columns():
            more = jnp.dot(z, ws[final, :, cols], preferred_element_type=F32)
            out_skip[s, :, cols] = (skip[s, :, cols] + more).astype(BF16)

    @pl.when(me + 1 < n)
    def _():
        for layer in range(near):
            for s in every:
                send(layer, s).wait_send()

    for route in routes.values():
        for ok, slot, block, where, other in route:

            @pl.when(ok)
            def _(slot=slot, block=block, where=where, other=other):
                for s in every:
                    ship(slot, s, block, where, other).wait_send()


def fused(n, signal, taps, w_gate, w_res, w_skip):
    seqs, length, width = signal.shape
    layers = taps.shape[0]
    near = length.bit_length() - 1
    halos = [pltpu.VMEM((seqs, max(ALIGN, 2**layer), width), BF16) for layer in range(near)]
    flops = 2 * seqs * length * width * width * 4 * layers
    in_vmem, anywhere = pl.BlockSpec(memory_space=pltpu.VMEM), pl.BlockSpec(memory_space=pl.ANY)
    return pl.pallas_call(
        functools.partial(kernel, n, layers, near),
        out_shape=[pltpu.VMEM(signal.shape, BF16)] * 2,
        in_specs=[anywhere] * 5,
        out_specs=[in_vmem, in_vmem],
        scratch_shapes=[
            pltpu.VMEM(signal.shape, BF16),
            pltpu.VMEM(taps.shape, F32),
            pltpu.VMEM((layers, width, 2, width), BF16),
            pltpu.VMEM((layers, 2, width, width), BF16),
            pltpu.VMEM((layers, width, width), BF16),
            pltpu.VMEM((layers, width, width), BF16),
            pltpu.VMEM((layers - 1, seqs, length, width), BF16),
            pltpu.VMEM((layers - 1, seqs, length, width), BF16),
            pltpu.VMEM((seqs, length, width), F32),
            pltpu.VMEM((seqs, length, width), BF16),
            pltpu.VMEM((5, seqs, length, width), BF16),
            pltpu.SemaphoreType.DMA((2,)),
            pltpu.SemaphoreType.DMA((layers, 3)),
            pltpu.SemaphoreType.DMA((near, seqs)),
            pltpu.SemaphoreType.DMA((near, seqs)),
            pltpu.SemaphoreType.DMA((6, seqs)),
            pltpu.SemaphoreType.DMA((5, seqs)),
            pltpu.SemaphoreType.REGULAR,
            *halos,
        ],
        compiler_params=pltpu.CompilerParams(collective_id=0, has_side_effects=True, vmem_limit_bytes=VMEM_LIMIT),
        cost_estimate=pl.CostEstimate(flops=flops, bytes_accessed=8 * layers * width * width, transcendentals=0),
        name="stack",
    )(signal, taps, w_gate, w_res, w_skip)


def solution(mesh):
    in_specs = (
        P(None, "tm", "chan"),
        P(None, None, "chan"),
        P(None, None, None, "chan"),
        P(None, None, "chan"),
        P(None, None, "chan"),
    )
    out_specs = (P(None, "tm", "chan"), P(None, "tm", "chan"))

    def body(*args):
        n, length, layers = mesh.shape["tm"], args[0].shape[1], args[1].shape[0]
        fits = length >= 4 * ALIGN and 2 ** (layers - 3) == length and n % 4 == 0
        if mesh.shape["chan"] == 1 and fits:
            return tuple(fused(n, *args))
        return local(*args)

    return jax.shard_map(body, mesh=mesh, in_specs=in_specs, out_specs=out_specs, check_vma=False)
```

```python
import functools

import jax
import jax.numpy as jnp
from jax import lax
from jax.experimental import pallas as pl
from jax.experimental.pallas import tpu as pltpu
from jax.sharding import PartitionSpec as P

MESH = pl.DeviceIdType.MESH
BF16, F32 = jnp.bfloat16, jnp.float32
ALIGN = 16
VMEM_LIMIT = 56000 * 1024


def shifted(value, axis, steps):
    count = lax.axis_size(axis)
    leading, last = (max(0, -steps), min(count, count - steps))
    return lax.ppermute(value, axis, [(source, source + steps) for source in range(leading, last)])


def delay_block(stream, delay, near_fn, far_fn):
    length = stream.shape[1]
    whole, rest = divmod(delay, length)
    if whole == 0:
        nearer = stream
    else:
        nearer = near_fn(stream, whole)
    if rest == 0:
        return nearer
    farther = far_fn(stream[:, length - rest :], whole + 1)
    return jnp.concatenate([farther, nearer[:, : length - rest]], axis=1)


def near_time(block, steps):
    return shifted(block, "tm", steps)


def far_time(block, steps):
    return shifted(block, "tm", steps)


def gate_units(hidden):
    return (jnp.tanh(hidden[:, :, 0]) * jax.nn.sigmoid(hidden[:, :, 1])).astype(jnp.bfloat16)


def local(signal, taps, w_gate, w_res, w_skip):
    stream = signal
    seqs, length, local_c = stream.shape
    skip = jnp.zeros((seqs, length, local_c), jnp.float32)
    for layer in range(taps.shape[0]):
        delayed = delay_block(stream, 2**layer, near_time, far_time)
        conv = (
            taps[layer, 0] * delayed.astype(jnp.float32)
            + taps[layer, 1] * stream.astype(jnp.float32)
        ).astype(jnp.bfloat16)
        gate_w = w_gate[layer]
        hidden = jnp.einsum(
            "stc,cko->stko",
            lax.all_gather(conv, "chan", axis=2, tiled=True),
            gate_w,
            preferred_element_type=jnp.float32,
        )
        gated = gate_units(hidden)
        res_w = w_res[layer]
        skip_w = w_skip[layer]
        piece = lax.all_gather(gated, "chan", axis=2, tiled=True)
        update = jnp.einsum("stc,co->sto", piece, res_w, preferred_element_type=jnp.float32)
        skip_part = jnp.einsum("stc,co->sto", piece, skip_w, preferred_element_type=jnp.float32)
        stream = (stream.astype(jnp.float32) + update).astype(jnp.bfloat16)
        skip = skip + skip_part
    return (stream, skip.astype(jnp.bfloat16))


def tanh_gate(filt, gate):
    return (jnp.tanh(filt) * (0.5 * jnp.tanh(0.5 * gate) + 0.5)).astype(BF16)


def pair_order(block):
    row = lax.broadcasted_iota(jnp.int32, (2 * block, 2 * block), 0)
    column = lax.broadcasted_iota(jnp.int32, (2 * block, 2 * block), 1)
    wanted = jnp.where(row < block, 2 * row, 2 * (row - block) + 1)
    return jnp.where(column == wanted, 1.0, 0.0).astype(F32).astype(BF16)


def split_pairs(pairs, out, order, blocks):
    block = order.shape[0] // 2
    for index in blocks:
        at = index * block
        both = pairs[at : at + block].reshape(2 * block, pairs.shape[2])
        sorted_rows = jnp.dot(order, both, preferred_element_type=F32).astype(BF16)
        out[0, at : at + block] = sorted_rows[:block]
        out[1, at : at + block] = sorted_rows[block:]


P1, P2, P3, P4, P9 = range(5)
REACH = 4


def kernel(n, layers, near, sig_hbm, taps_hbm, wg_hbm, wr_hbm, ws_hbm, out_x, out_skip, *scratch):
    sig, taps, raw, wg, wr, ws, xs, zs, skip, ahead, far = scratch[:11]
    in_sem, w_sem, send_sem, recv_sem, far_send, far_recv, order_sem = scratch[11:18]
    halos = scratch[18:]
    seqs, length, width = sig.shape
    me = lax.axis_index("tm")
    place = lax.rem(me, 4)
    core = lax.rem(me, 2)
    clean = near - 1
    rows_of = [max(ALIGN, 2**layer) for layer in range(near)]
    half = min(256, width)
    every = list(range(seqs))

    def fence():
        pl.semaphore_signal(order_sem, 1)
        pl.semaphore_wait(order_sem, 1)

    def weights(layer):
        return [
            pltpu.make_async_copy(wg_hbm.at[layer], raw.at[layer], w_sem.at[layer, 0]),
            pltpu.make_async_copy(wr_hbm.at[layer], wr.at[layer], w_sem.at[layer, 1]),
            pltpu.make_async_copy(ws_hbm.at[layer], ws.at[layer], w_sem.at[layer, 2]),
        ]

    inputs = [
        pltpu.make_async_copy(sig_hbm, sig, in_sem.at[0]),
        pltpu.make_async_copy(taps_hbm, taps, in_sem.at[1]),
    ]
    for copy in inputs:
        copy.start()
    fence()
    for layer in range(layers):
        for copy in weights(layer):
            copy.start()

    barrier = pltpu.get_barrier_semaphore()
    for step in range(1, REACH + 1):
        for ok, other in ((me + step < n, me + step), (me >= step, me - step)):

            @pl.when(ok)
            def _(other=other):
                pl.semaphore_signal(barrier, inc=1, device_id={"tm": other}, device_id_type=MESH)

    def source(layer):
        return sig if layer == 0 else xs.at[layer - 1]

    def send(layer, s):
        rows = rows_of[layer]
        return pltpu.make_async_remote_copy(
            src_ref=source(layer).at[s, pl.ds(length - rows, rows)],
            dst_ref=halos[layer].at[s],
            send_sem=send_sem.at[layer, s],
            recv_sem=recv_sem.at[layer, s],
            device_id={"tm": me + 1},
            device_id_type=MESH,
        )

    def start_send(layer):
        @pl.when(me + 1 < n)
        def _():
            for s in every:
                send(layer, s).start()

    def take(layer, which):
        @pl.when(me >= 1)
        def _():
            for s in which:
                send(layer, s).wait_recv()

        @pl.when(me < 1)
        def _():
            for s in which:
                halos[layer][s] = jnp.zeros(halos[layer].shape[1:], BF16)

    def ship(slot, s, block, where, other):
        return pltpu.make_async_remote_copy(
            src_ref=block.at[s],
            dst_ref=far.at[where, s],
            send_sem=far_send.at[slot, s],
            recv_sem=far_recv.at[where, s],
            device_id={"tm": other},
            device_id_type=MESH,
        )

    last_near, last_far = xs.at[near - 1], xs.at[layers - 2]
    relay = (place == 3) & (me >= 7)
    routes = {
        "own": [
            ((place == 3) & (me + 4 < n), 0, last_near, P4, me + 4),
            ((place != 3) & (me + 2 < n), 0, last_near, P2, me + 2),
            ((place == 1) & (me + 3 < n), 1, last_near, P3, me + 3),
            (core == 0, 1, last_near, P1, me + 1),
        ],
        "relay": [
            (relay, 2, far.at[P4], P2, me - 2),
            (relay, 3, far.at[P4], P3, me - 1),
        ],
        "share": [
            ((core == 1) & (me >= 2), 4, far.at[P2], P1, me - 1),
            ((core == 0) & (me >= 2), 4, far.at[P2], P3, me + 1),
        ],
        "last": [(me + 4 < n, 5, last_far, P9, me + 4)],
    }

    def go(kind, s):
        for ok, slot, block, where, other in routes[kind]:

            @pl.when(ok)
            def _(slot=slot, block=block, where=where, other=other):
                ship(slot, s, block, where, other).start()

    def get(where, s, least):
        @pl.when(me >= least)
        def _():
            ship(0, s, last_near, where, me).wait_recv()

        @pl.when(me < least)
        def _():
            far[where, s] = jnp.zeros(far.shape[2:], BF16)

    def load(layer, s, low, high):
        return source(layer)[s, low:high]

    def stack(parts):
        return jnp.concatenate(parts, axis=0) if len(parts) > 1 else parts[0]

    def gated(layer, late, own_f):
        conv = (taps[layer, 0:1] * late.astype(F32) + taps[layer, 1:2] * own_f).astype(BF16)
        parts = []
        for at in range(0, width, half):
            filt = jnp.dot(conv, wg[layer, 0, :, at : at + half], preferred_element_type=F32)
            gate = jnp.dot(conv, wg[layer, 1, :, at : at + half], preferred_element_type=F32)
            parts.append(tanh_gate(filt, gate))
        return jnp.concatenate(parts, axis=1) if len(parts) > 1 else parts[0]

    def columns():
        return [slice(at, at + half) for at in range(0, width, half)]

    def renewed(layer, z, own_f, cols):
        return (own_f[:, cols] + jnp.dot(z, wr[layer, :, cols], preferred_element_type=F32)).astype(BF16)

    def finish(layer, delayed, own, which, low, high, before=None, between=None):
        count = high - low
        if before:
            before()
        own_f = stack(own).astype(F32)
        z = gated(layer, stack(delayed), own_f)
        for i, s in enumerate(which):
            zs[layer, s, low:high] = z[i * count : (i + 1) * count]
        if between:
            between()
        for cols in columns():
            new = renewed(layer, z, own_f, cols)
            for i, s in enumerate(which):
                xs[layer, s, low:high, cols] = new[i * count : (i + 1) * count]

    top = [max(ALIGN, 2 ** (layer + 1)) for layer in range(clean)]
    first = [0] * clean
    for layer in range(clean - 1, -1, -1):
        need = top[layer] if layer == clean - 1 else first[layer + 1] - 2 ** (layer + 1)
        first[layer] = max(0, min(need, top[layer]) // ALIGN * ALIGN)

    block = min(128, width)
    order = pair_order(block)
    blocks = list(range(width // block))

    def landed(layer):
        for copy in weights(layer):
            copy.wait()

    def split(layer, which):
        split_pairs(raw.at[layer], wg.at[layer], order, which)

    def arrive(layer):
        landed(layer)
        split(layer, blocks)

    for copy in inputs:
        copy.wait()
    arrive(0)
    early, late_blocks = blocks[: len(blocks) // 2], blocks[len(blocks) // 2 :]
    for layer in range(clean):
        delay, low = 2**layer, first[layer]
        landed(layer + 1)
        delayed, own = [], []
        for s in every:
            if delay < ALIGN:
                begin = max(0, low - ALIGN)
                block = pltpu.roll(load(layer, s, begin, length).astype(F32), delay, 0)
                delayed.append(block[low - begin :])
            else:
                delayed.append(load(layer, s, low - delay, length - delay))
            own.append(load(layer, s, low, length))
        finish(
            layer, delayed, own, every, low, length,
            lambda: split(layer + 1, early), lambda: split(layer + 1, late_blocks),
        )
        if layer == 0:
            total = sum(
                ((me + step < n).astype(jnp.int32) + (me >= step).astype(jnp.int32)) for step in range(1, REACH + 1)
            )
            pl.semaphore_wait(barrier, total)
            start_send(0)
        start_send(layer + 1)

    for layer in range(clean):
        delay, high = 2**layer, top[layer]
        take(layer, every)
        delayed, own = [], []
        for s in every:
            rows = rows_of[layer]
            tail = halos[layer][s]
            if delay < ALIGN:
                joined = jnp.concatenate([tail.astype(F32), load(layer, s, 0, high).astype(F32)], axis=0)
                delayed.append(pltpu.roll(joined, delay, 0)[rows:])
            else:
                delayed.append(jnp.concatenate([tail, load(layer, s, 0, high - delay)], axis=0))
            own.append(load(layer, s, 0, high))
        finish(layer, delayed, own, every, 0, high)

    for s in every:
        take(clean, [s])
        late = jnp.concatenate([halos[clean][s], load(clean, s, 0, length - 2**clean)], axis=0)
        finish(clean, [late], [load(clean, s, 0, length)], [s], 0, length)
        go("own", s)

    for layer in range(near, layers):
        arrive(layer)

    def held_skip(span):
        for cols in columns():
            total = None
            for before in span:
                z = zs[before].reshape(seqs * length, width)
                more = jnp.dot(z, ws[before, :, cols], preferred_element_type=F32)
                total = more if total is None else total + more
            total = total.reshape(seqs, length, half)
            skip[:, :, cols] = total if span[0] == 0 else skip[:, :, cols] + total

    for s in every:

        @pl.when(relay)
        def _(s=s):
            ship(0, s, last_near, P4, me).wait_recv()

        go("relay", s)
        if s < seqs - 1:
            held_skip(range(near * s // (seqs - 1), near * (s + 1) // (seqs - 1)))

    for s in every:
        get(P2, s, 2)
        go("share", s)
        get(P1, s, 1)
        get(P3, s, 3)
        late = jnp.concatenate([far[P1, s], far[P3, s]], axis=0)
        own_f = jnp.concatenate([xs[near - 1, s], far[P2, s]], axis=0).astype(F32)
        z = gated(near, late, own_f)
        zs[near, s] = z[:length]
        for cols in columns():
            new = renewed(near, z, own_f, cols)
            xs[near, s, :, cols] = new[:length]
            ahead[s, :, cols] = new[length:]
        own_f = xs[near, s].astype(F32)
        z = gated(near + 1, ahead[s], own_f)
        zs[near + 1, s] = z
        for cols in columns():
            xs[near + 1, s, :, cols] = renewed(near + 1, z, own_f, cols)
        go("last", s)

    held_skip(range(near, layers - 1))

    final = layers - 1
    for s in every:
        get(P9, s, 4)
        own_f = xs[final - 1, s].astype(F32)
        z = gated(final, far[P9, s], own_f)
        for cols in columns():
            out_x[s, :, cols] = renewed(final, z, own_f, cols)
        for cols in columns():
            more = jnp.dot(z, ws[final, :, cols], preferred_element_type=F32)
            out_skip[s, :, cols] = (skip[s, :, cols] + more).astype(BF16)

    @pl.when(me + 1 < n)
    def _():
        for layer in range(near):
            for s in every:
                send(layer, s).wait_send()

    for route in routes.values():
        for ok, slot, block, where, other in route:

            @pl.when(ok)
            def _(slot=slot, block=block, where=where, other=other):
                for s in every:
                    ship(slot, s, block, where, other).wait_send()


def fused(n, signal, taps, w_gate, w_res, w_skip):
    seqs, length, width = signal.shape
    layers = taps.shape[0]
    near = length.bit_length() - 1
    halos = [pltpu.VMEM((seqs, max(ALIGN, 2**layer), width), BF16) for layer in range(near)]
    flops = 2 * seqs * length * width * width * 4 * layers
    in_vmem, anywhere = pl.BlockSpec(memory_space=pltpu.VMEM), pl.BlockSpec(memory_space=pl.ANY)
    return pl.pallas_call(
        functools.partial(kernel, n, layers, near),
        out_shape=[pltpu.VMEM(signal.shape, BF16)] * 2,
        in_specs=[anywhere] * 5,
        out_specs=[in_vmem, in_vmem],
        scratch_shapes=[
            pltpu.VMEM(signal.shape, BF16),
            pltpu.VMEM(taps.shape, F32),
            pltpu.VMEM((layers, width, 2, width), BF16),
            pltpu.VMEM((layers, 2, width, width), BF16),
            pltpu.VMEM((layers, width, width), BF16),
            pltpu.VMEM((layers, width, width), BF16),
            pltpu.VMEM((layers - 1, seqs, length, width), BF16),
            pltpu.VMEM((layers - 1, seqs, length, width), BF16),
            pltpu.VMEM((seqs, length, width), F32),
            pltpu.VMEM((seqs, length, width), BF16),
            pltpu.VMEM((5, seqs, length, width), BF16),
            pltpu.SemaphoreType.DMA((2,)),
            pltpu.SemaphoreType.DMA((layers, 3)),
            pltpu.SemaphoreType.DMA((near, seqs)),
            pltpu.SemaphoreType.DMA((near, seqs)),
            pltpu.SemaphoreType.DMA((6, seqs)),
            pltpu.SemaphoreType.DMA((5, seqs)),
            pltpu.SemaphoreType.REGULAR,
            *halos,
        ],
        compiler_params=pltpu.CompilerParams(collective_id=0, has_side_effects=True, vmem_limit_bytes=VMEM_LIMIT),
        cost_estimate=pl.CostEstimate(flops=flops, bytes_accessed=8 * layers * width * width, transcendentals=0),
        name="stack",
    )(signal, taps, w_gate, w_res, w_skip)


def solution(mesh):
    in_specs = (
        P(None, "tm", "chan"),
        P(None, None, "chan"),
        P(None, None, None, "chan"),
        P(None, None, "chan"),
        P(None, None, "chan"),
    )
    out_specs = (P(None, "tm", "chan"), P(None, "tm", "chan"))

    def body(*args):
        n, length, layers = mesh.shape["tm"], args[0].shape[1], args[1].shape[0]
        fits = length >= 4 * ALIGN and 2 ** (layers - 3) == length and n % 4 == 0
        if mesh.shape["chan"] == 1 and fits:
            return tuple(fused(n, *args))
        return local(*args)

    return jax.shard_map(body, mesh=mesh, in_specs=in_specs, out_specs=out_specs, check_vma=False)
```

```python
import functools

import jax
import jax.numpy as jnp
from jax import lax
from jax.experimental import pallas as pl
from jax.experimental.pallas import tpu as pltpu
from jax.sharding import PartitionSpec as P

MESH = pl.DeviceIdType.MESH
BF16, F32 = jnp.bfloat16, jnp.float32
ALIGN = 16
VMEM_LIMIT = 56000 * 1024


def shifted(value, axis, steps):
    count = lax.axis_size(axis)
    leading, last = (max(0, -steps), min(count, count - steps))
    return lax.ppermute(value, axis, [(source, source + steps) for source in range(leading, last)])


def delay_block(stream, delay, near_fn, far_fn):
    length = stream.shape[1]
    whole, rest = divmod(delay, length)
    if whole == 0:
        nearer = stream
    else:
        nearer = near_fn(stream, whole)
    if rest == 0:
        return nearer
    farther = far_fn(stream[:, length - rest :], whole + 1)
    return jnp.concatenate([farther, nearer[:, : length - rest]], axis=1)


def near_time(block, steps):
    return shifted(block, "tm", steps)


def far_time(block, steps):
    return shifted(block, "tm", steps)


def gate_units(hidden):
    return (jnp.tanh(hidden[:, :, 0]) * jax.nn.sigmoid(hidden[:, :, 1])).astype(jnp.bfloat16)


def local(signal, taps, w_gate, w_res, w_skip):
    stream = signal
    seqs, length, local_c = stream.shape
    skip = jnp.zeros((seqs, length, local_c), jnp.float32)
    for layer in range(taps.shape[0]):
        delayed = delay_block(stream, 2**layer, near_time, far_time)
        conv = (
            taps[layer, 0] * delayed.astype(jnp.float32)
            + taps[layer, 1] * stream.astype(jnp.float32)
        ).astype(jnp.bfloat16)
        gate_w = w_gate[layer]
        hidden = jnp.einsum(
            "stc,cko->stko",
            lax.all_gather(conv, "chan", axis=2, tiled=True),
            gate_w,
            preferred_element_type=jnp.float32,
        )
        gated = gate_units(hidden)
        res_w = w_res[layer]
        skip_w = w_skip[layer]
        piece = lax.all_gather(gated, "chan", axis=2, tiled=True)
        update = jnp.einsum("stc,co->sto", piece, res_w, preferred_element_type=jnp.float32)
        skip_part = jnp.einsum("stc,co->sto", piece, skip_w, preferred_element_type=jnp.float32)
        stream = (stream.astype(jnp.float32) + update).astype(jnp.bfloat16)
        skip = skip + skip_part
    return (stream, skip.astype(jnp.bfloat16))


def tanh_gate(filt, gate):
    return (jnp.tanh(filt) * (0.5 * jnp.tanh(0.5 * gate) + 0.5)).astype(BF16)


def pair_order(block):
    row = lax.broadcasted_iota(jnp.int32, (2 * block, 2 * block), 0)
    column = lax.broadcasted_iota(jnp.int32, (2 * block, 2 * block), 1)
    wanted = jnp.where(row < block, 2 * row, 2 * (row - block) + 1)
    return jnp.where(column == wanted, 1.0, 0.0).astype(F32).astype(BF16)


def split_pairs(pairs, out, order, blocks):
    block = order.shape[0] // 2
    for index in blocks:
        at = index * block
        both = pairs[at : at + block].reshape(2 * block, pairs.shape[2])
        sorted_rows = jnp.dot(order, both, preferred_element_type=F32).astype(BF16)
        out[0, at : at + block] = sorted_rows[:block]
        out[1, at : at + block] = sorted_rows[block:]


P1, P2, P3, P4, P9 = range(5)
REACH = 4


def kernel(n, layers, near, sig_hbm, taps_hbm, wg_hbm, wr_hbm, ws_hbm, out_x, out_skip, *scratch):
    sig, taps, raw, wg, wr, ws, xs, zs, skip, ahead, far = scratch[:11]
    in_sem, w_sem, send_sem, recv_sem, far_send, far_recv, order_sem = scratch[11:18]
    halos = scratch[18:]
    seqs, length, width = sig.shape
    me = lax.axis_index("tm")
    place = lax.rem(me, 4)
    core = lax.rem(me, 2)
    clean = near - 1
    rows_of = [max(ALIGN, 2**layer) for layer in range(near)]
    half = min(256, width)
    every = list(range(seqs))

    def fence():
        pl.semaphore_signal(order_sem, 1)
        pl.semaphore_wait(order_sem, 1)

    def weights(layer):
        return [
            pltpu.make_async_copy(wg_hbm.at[layer], raw.at[layer], w_sem.at[layer, 0]),
            pltpu.make_async_copy(wr_hbm.at[layer], wr.at[layer], w_sem.at[layer, 1]),
            pltpu.make_async_copy(ws_hbm.at[layer], ws.at[layer], w_sem.at[layer, 2]),
        ]

    inputs = [
        pltpu.make_async_copy(sig_hbm, sig, in_sem.at[0]),
        pltpu.make_async_copy(taps_hbm, taps, in_sem.at[1]),
    ]
    weights(0)[0].start()
    fence()
    for copy in inputs:
        copy.start()
    fence()
    weights(0)[1].start()
    fence()
    for layer in range(1, layers):
        for copy in weights(layer)[:2]:
            copy.start()
        if layer <= near:
            fence()
    fence()
    for layer in range(layers):
        weights(layer)[2].start()

    barrier = pltpu.get_barrier_semaphore()
    for step in range(1, REACH + 1):
        for ok, other in ((me + step < n, me + step), (me >= step, me - step)):

            @pl.when(ok)
            def _(other=other):
                pl.semaphore_signal(barrier, inc=1, device_id={"tm": other}, device_id_type=MESH)

    def source(layer):
        return sig if layer == 0 else xs.at[layer - 1]

    def send(layer, s):
        rows = rows_of[layer]
        return pltpu.make_async_remote_copy(
            src_ref=source(layer).at[s, pl.ds(length - rows, rows)],
            dst_ref=halos[layer].at[s],
            send_sem=send_sem.at[layer, s],
            recv_sem=recv_sem.at[layer, s],
            device_id={"tm": me + 1},
            device_id_type=MESH,
        )

    def start_send(layer):
        @pl.when(me + 1 < n)
        def _():
            for s in every:
                send(layer, s).start()

    def take(layer, which):
        @pl.when(me >= 1)
        def _():
            for s in which:
                send(layer, s).wait_recv()

        @pl.when(me < 1)
        def _():
            for s in which:
                halos[layer][s] = jnp.zeros(halos[layer].shape[1:], BF16)

    def ship(slot, s, block, where, other):
        return pltpu.make_async_remote_copy(
            src_ref=block.at[s],
            dst_ref=far.at[where, s],
            send_sem=far_send.at[slot, s],
            recv_sem=far_recv.at[where, s],
            device_id={"tm": other},
            device_id_type=MESH,
        )

    last_near, last_far = xs.at[near - 1], xs.at[layers - 2]
    relay = (place == 3) & (me >= 7)
    routes = {
        "own": [
            ((place == 3) & (me + 4 < n), 0, last_near, P4, me + 4),
            ((place != 3) & (me + 2 < n), 0, last_near, P2, me + 2),
            ((place == 1) & (me + 3 < n), 1, last_near, P3, me + 3),
            (core == 0, 1, last_near, P1, me + 1),
        ],
        "relay": [
            (relay, 2, far.at[P4], P2, me - 2),
            (relay, 3, far.at[P4], P3, me - 1),
        ],
        "share": [
            ((place == 1) & (me >= 2), 4, far.at[P2], P1, me - 1),
            ((core == 0) & (me >= 2), 4, far.at[P2], P3, me + 1),
        ],
        "early": [(place == 3, 4, far.at[P2], P1, me - 1)],
        "last": [(me + 4 < n, 5, last_far, P9, me + 4)],
    }

    def go(kind, s):
        for ok, slot, block, where, other in routes[kind]:

            @pl.when(ok)
            def _(slot=slot, block=block, where=where, other=other):
                ship(slot, s, block, where, other).start()

    def get(where, s, least):
        @pl.when(me >= least)
        def _():
            ship(0, s, last_near, where, me - 1).wait_recv()

        @pl.when(me < least)
        def _():
            far[where, s] = jnp.zeros(far.shape[2:], BF16)

    def load(layer, s, low, high):
        return source(layer)[s, low:high]

    def stack(parts):
        return jnp.concatenate(parts, axis=0) if len(parts) > 1 else parts[0]

    def gated(layer, late, own_f):
        conv = (taps[layer, 0:1] * late.astype(F32) + taps[layer, 1:2] * own_f).astype(BF16)
        parts = []
        for at in range(0, width, half):
            filt = jnp.dot(conv, wg[layer, 0, :, at : at + half], preferred_element_type=F32)
            gate = jnp.dot(conv, wg[layer, 1, :, at : at + half], preferred_element_type=F32)
            parts.append(tanh_gate(filt, gate))
        return jnp.concatenate(parts, axis=1) if len(parts) > 1 else parts[0]

    def columns():
        return [slice(at, at + half) for at in range(0, width, half)]

    def renewed(layer, z, own_f, cols):
        return (own_f[:, cols] + jnp.dot(z, wr[layer, :, cols], preferred_element_type=F32)).astype(BF16)

    def finish(layer, delayed, own, which, low, high, before=None, between=None):
        count = high - low
        if before:
            before()
        own_f = stack(own).astype(F32)
        z = gated(layer, stack(delayed), own_f)
        for i, s in enumerate(which):
            zs[layer, s, low:high] = z[i * count : (i + 1) * count]
        if between:
            between()
        for cols in columns():
            new = renewed(layer, z, own_f, cols)
            for i, s in enumerate(which):
                xs[layer, s, low:high, cols] = new[i * count : (i + 1) * count]

    top = [max(ALIGN, 2 ** (layer + 1)) for layer in range(clean)]
    first = [0] * clean
    for layer in range(clean - 1, -1, -1):
        need = top[layer] if layer == clean - 1 else first[layer + 1] - 2 ** (layer + 1)
        first[layer] = max(0, min(need, top[layer]) // ALIGN * ALIGN)

    block = min(128, width)
    order = pair_order(block)
    blocks = list(range(width // block))

    def landed(layer):
        for copy in weights(layer)[:2]:
            copy.wait()

    def split(layer, which):
        split_pairs(raw.at[layer], wg.at[layer], order, which)

    def arrive(layer):
        landed(layer)
        split(layer, blocks)

    weights(0)[0].wait()
    split(0, blocks)
    for copy in inputs:
        copy.wait()
    weights(0)[1].wait()
    early, late_blocks = blocks[: len(blocks) // 2], blocks[len(blocks) // 2 :]
    for layer in range(clean):
        delay, low = 2**layer, first[layer]
        landed(layer + 1)
        delayed, own = [], []
        for s in every:
            if delay < ALIGN:
                begin = max(0, low - ALIGN)
                block = pltpu.roll(load(layer, s, begin, length).astype(F32), delay, 0)
                delayed.append(block[low - begin :])
            else:
                delayed.append(load(layer, s, low - delay, length - delay))
            own.append(load(layer, s, low, length))
        finish(
            layer, delayed, own, every, low, length,
            lambda: split(layer + 1, early), lambda: split(layer + 1, late_blocks),
        )
        if layer == 0:
            total = sum(
                ((me + step < n).astype(jnp.int32) + (me >= step).astype(jnp.int32)) for step in range(1, REACH + 1)
            )
            pl.semaphore_wait(barrier, total)
            start_send(0)
        start_send(layer + 1)

    for layer in range(clean):
        delay, high = 2**layer, top[layer]
        take(layer, every)
        delayed, own = [], []
        for s in every:
            rows = rows_of[layer]
            tail = halos[layer][s]
            if delay < ALIGN:
                joined = jnp.concatenate([tail.astype(F32), load(layer, s, 0, high).astype(F32)], axis=0)
                delayed.append(pltpu.roll(joined, delay, 0)[rows:])
            else:
                delayed.append(jnp.concatenate([tail, load(layer, s, 0, high - delay)], axis=0))
            own.append(load(layer, s, 0, high))
        finish(layer, delayed, own, every, 0, high)

    for s in every:
        take(clean, [s])
        late = jnp.concatenate([halos[clean][s], load(clean, s, 0, length - 2**clean)], axis=0)
        finish(clean, [late], [load(clean, s, 0, length)], [s], 0, length)
        go("own", s)

    def early(s):
        @pl.when(place == 3)
        def _():
            ship(0, s, last_near, P2, me - 2).wait_recv()
            ship(4, s, far.at[P2], P1, me - 1).start()

        @pl.when(relay)
        def _():
            ship(0, s, last_near, P4, me - 2).wait_recv()

        go("relay", s)

    def share(s):
        @pl.when((place != 3) & (me >= 2))
        def _():
            ship(0, s, last_near, P2, me - 2).wait_recv()

        @pl.when(me < 2)
        def _():
            far[P2, s] = jnp.zeros(far.shape[2:], BF16)

        go("share", s)

    def held_skip(span):
        for cols in columns():
            total = None
            for before in span:
                z = zs[before].reshape(seqs * length, width)
                more = jnp.dot(z, ws[before, :, cols], preferred_element_type=F32)
                total = more if total is None else total + more
            total = total.reshape(seqs, length, half)
            skip[:, :, cols] = total if span[0] == 0 else skip[:, :, cols] + total

    arrive(near)
    arrive(near + 1)
    early(0)
    for layer in range(near + 2, layers):
        arrive(layer)
    for layer in range(layers):
        weights(layer)[2].wait()
    held_skip(range(near))

    for s in every:
        if s + 1 < seqs:
            early(s + 1)
        share(s)
        get(P1, s, 1)
        get(P3, s, 3)
        late = jnp.concatenate([far[P1, s], far[P3, s]], axis=0)
        own_f = jnp.concatenate([xs[near - 1, s], far[P2, s]], axis=0).astype(F32)
        z = gated(near, late, own_f)
        zs[near, s] = z[:length]
        for cols in columns():
            new = renewed(near, z, own_f, cols)
            xs[near, s, :, cols] = new[:length]
            ahead[s, :, cols] = new[length:]
        own_f = xs[near, s].astype(F32)
        z = gated(near + 1, ahead[s], own_f)
        zs[near + 1, s] = z
        for cols in columns():
            xs[near + 1, s, :, cols] = renewed(near + 1, z, own_f, cols)
        go("last", s)

    held_skip(range(near, layers - 1))

    final = layers - 1
    for s in every:
        get(P9, s, 4)
        own_f = xs[final - 1, s].astype(F32)
        z = gated(final, far[P9, s], own_f)
        for cols in columns():
            out_x[s, :, cols] = renewed(final, z, own_f, cols)
        for cols in columns():
            more = jnp.dot(z, ws[final, :, cols], preferred_element_type=F32)
            out_skip[s, :, cols] = (skip[s, :, cols] + more).astype(BF16)

    @pl.when(me + 1 < n)
    def _():
        for layer in range(near):
            for s in every:
                send(layer, s).wait_send()

    for route in routes.values():
        for ok, slot, block, where, other in route:

            @pl.when(ok)
            def _(slot=slot, block=block, where=where, other=other):
                for s in every:
                    ship(slot, s, block, where, other).wait_send()


def fused(n, signal, taps, w_gate, w_res, w_skip):
    seqs, length, width = signal.shape
    layers = taps.shape[0]
    near = length.bit_length() - 1
    halos = [pltpu.VMEM((seqs, max(ALIGN, 2**layer), width), BF16) for layer in range(near)]
    flops = 2 * seqs * length * width * width * 4 * layers
    in_vmem, anywhere = pl.BlockSpec(memory_space=pltpu.VMEM), pl.BlockSpec(memory_space=pl.ANY)
    return pl.pallas_call(
        functools.partial(kernel, n, layers, near),
        out_shape=[pltpu.VMEM(signal.shape, BF16)] * 2,
        in_specs=[anywhere] * 5,
        out_specs=[in_vmem, in_vmem],
        scratch_shapes=[
            pltpu.VMEM(signal.shape, BF16),
            pltpu.VMEM(taps.shape, F32),
            pltpu.VMEM((layers, width, 2, width), BF16),
            pltpu.VMEM((layers, 2, width, width), BF16),
            pltpu.VMEM((layers, width, width), BF16),
            pltpu.VMEM((layers, width, width), BF16),
            pltpu.VMEM((layers - 1, seqs, length, width), BF16),
            pltpu.VMEM((layers - 1, seqs, length, width), BF16),
            pltpu.VMEM((seqs, length, width), F32),
            pltpu.VMEM((seqs, length, width), BF16),
            pltpu.VMEM((5, seqs, length, width), BF16),
            pltpu.SemaphoreType.DMA((2,)),
            pltpu.SemaphoreType.DMA((layers, 3)),
            pltpu.SemaphoreType.DMA((near, seqs)),
            pltpu.SemaphoreType.DMA((near, seqs)),
            pltpu.SemaphoreType.DMA((6, seqs)),
            pltpu.SemaphoreType.DMA((5, seqs)),
            pltpu.SemaphoreType.REGULAR,
            *halos,
        ],
        compiler_params=pltpu.CompilerParams(collective_id=0, has_side_effects=True, vmem_limit_bytes=VMEM_LIMIT),
        cost_estimate=pl.CostEstimate(flops=flops, bytes_accessed=8 * layers * width * width, transcendentals=0),
        name="stack",
    )(signal, taps, w_gate, w_res, w_skip)


def solution(mesh):
    in_specs = (
        P(None, "tm", "chan"),
        P(None, None, "chan"),
        P(None, None, None, "chan"),
        P(None, None, "chan"),
        P(None, None, "chan"),
    )
    out_specs = (P(None, "tm", "chan"), P(None, "tm", "chan"))

    def body(*args):
        n, length, layers = mesh.shape["tm"], args[0].shape[1], args[1].shape[0]
        fits = length >= 4 * ALIGN and 2 ** (layers - 3) == length and n % 4 == 0
        if mesh.shape["chan"] == 1 and fits:
            return tuple(fused(n, *args))
        return local(*args)

    return jax.shard_map(body, mesh=mesh, in_specs=in_specs, out_specs=out_specs, check_vma=False)
```

```python
import functools

import jax
import jax.numpy as jnp
from jax import lax
from jax.experimental import pallas as pl
from jax.experimental.pallas import tpu as pltpu
from jax.sharding import PartitionSpec as P

MESH = pl.DeviceIdType.MESH
BF16, F32 = jnp.bfloat16, jnp.float32
ALIGN = 16
VMEM_LIMIT = 56000 * 1024


def shifted(value, axis, steps):
    count = lax.axis_size(axis)
    leading, last = (max(0, -steps), min(count, count - steps))
    return lax.ppermute(value, axis, [(source, source + steps) for source in range(leading, last)])


def delay_block(stream, delay, near_fn, far_fn):
    length = stream.shape[1]
    whole, rest = divmod(delay, length)
    if whole == 0:
        nearer = stream
    else:
        nearer = near_fn(stream, whole)
    if rest == 0:
        return nearer
    farther = far_fn(stream[:, length - rest :], whole + 1)
    return jnp.concatenate([farther, nearer[:, : length - rest]], axis=1)


def near_time(block, steps):
    return shifted(block, "tm", steps)


def far_time(block, steps):
    return shifted(block, "tm", steps)


def gate_units(hidden):
    return (jnp.tanh(hidden[:, :, 0]) * jax.nn.sigmoid(hidden[:, :, 1])).astype(jnp.bfloat16)


def local(signal, taps, w_gate, w_res, w_skip):
    stream = signal
    seqs, length, local_c = stream.shape
    skip = jnp.zeros((seqs, length, local_c), jnp.float32)
    for layer in range(taps.shape[0]):
        delayed = delay_block(stream, 2**layer, near_time, far_time)
        conv = (
            taps[layer, 0] * delayed.astype(jnp.float32)
            + taps[layer, 1] * stream.astype(jnp.float32)
        ).astype(jnp.bfloat16)
        gate_w = w_gate[layer]
        hidden = jnp.einsum(
            "stc,cko->stko",
            lax.all_gather(conv, "chan", axis=2, tiled=True),
            gate_w,
            preferred_element_type=jnp.float32,
        )
        gated = gate_units(hidden)
        res_w = w_res[layer]
        skip_w = w_skip[layer]
        piece = lax.all_gather(gated, "chan", axis=2, tiled=True)
        update = jnp.einsum("stc,co->sto", piece, res_w, preferred_element_type=jnp.float32)
        skip_part = jnp.einsum("stc,co->sto", piece, skip_w, preferred_element_type=jnp.float32)
        stream = (stream.astype(jnp.float32) + update).astype(jnp.bfloat16)
        skip = skip + skip_part
    return (stream, skip.astype(jnp.bfloat16))


def tanh_gate(filt, gate):
    return (jnp.tanh(filt) * (0.5 * jnp.tanh(0.5 * gate) + 0.5)).astype(BF16)


def pair_order(block):
    row = lax.broadcasted_iota(jnp.int32, (2 * block, 2 * block), 0)
    column = lax.broadcasted_iota(jnp.int32, (2 * block, 2 * block), 1)
    wanted = jnp.where(row < block, 2 * row, 2 * (row - block) + 1)
    return jnp.where(column == wanted, 1.0, 0.0).astype(F32).astype(BF16)


def split_pairs(pairs, out, order, blocks):
    block = order.shape[0] // 2
    for index in blocks:
        at = index * block
        both = pairs[at : at + block].reshape(2 * block, pairs.shape[2])
        sorted_rows = jnp.dot(order, both, preferred_element_type=F32).astype(BF16)
        out[0, at : at + block] = sorted_rows[:block]
        out[1, at : at + block] = sorted_rows[block:]


P1, P2, P3, P4, P9 = range(5)
REACH = 4
PARTS = 2


def kernel(n, layers, near, sig_hbm, taps_hbm, wg_hbm, wr_hbm, ws_hbm, out_x, out_skip, *scratch):
    sig, taps, raw, wg, wr, ws, xs, zs, skip, ahead, far = scratch[:11]
    in_sem, w_sem, send_sem, recv_sem, far_send, far_recv, order_sem = scratch[11:18]
    halos = scratch[18:]
    seqs, length, width = sig.shape
    me = lax.axis_index("tm")
    place = lax.rem(me, 4)
    core = lax.rem(me, 2)
    clean = near - 1
    rows_of = [max(ALIGN, 2**layer) for layer in range(near)]
    half = min(256, width)
    every = list(range(seqs))

    def fence():
        pl.semaphore_signal(order_sem, 1)
        pl.semaphore_wait(order_sem, 1)

    def weights(layer):
        return [
            pltpu.make_async_copy(wg_hbm.at[layer], raw.at[layer], w_sem.at[layer, 0]),
            pltpu.make_async_copy(wr_hbm.at[layer], wr.at[layer], w_sem.at[layer, 1]),
            pltpu.make_async_copy(ws_hbm.at[layer], ws.at[layer], w_sem.at[layer, 2]),
        ]

    inputs = [
        pltpu.make_async_copy(sig_hbm, sig, in_sem.at[0]),
        pltpu.make_async_copy(taps_hbm, taps, in_sem.at[1]),
    ]
    weights(0)[0].start()
    fence()
    for copy in inputs:
        copy.start()
    fence()
    weights(0)[1].start()
    fence()
    for layer in range(1, layers):
        for copy in weights(layer)[:2]:
            copy.start()
        if layer <= near:
            fence()
    fence()
    for layer in range(layers):
        weights(layer)[2].start()

    barrier = pltpu.get_barrier_semaphore()
    for step in range(1, REACH + 1):
        for ok, other in ((me + step < n, me + step), (me >= step, me - step)):

            @pl.when(ok)
            def _(other=other):
                pl.semaphore_signal(barrier, inc=1, device_id={"tm": other}, device_id_type=MESH)

    def source(layer):
        return sig if layer == 0 else xs.at[layer - 1]

    def send(layer, s):
        rows = rows_of[layer]
        return pltpu.make_async_remote_copy(
            src_ref=source(layer).at[s, pl.ds(length - rows, rows)],
            dst_ref=halos[layer].at[s],
            send_sem=send_sem.at[layer, s],
            recv_sem=recv_sem.at[layer, s],
            device_id={"tm": me + 1},
            device_id_type=MESH,
        )

    def start_send(layer):
        @pl.when(me + 1 < n)
        def _():
            for s in every:
                send(layer, s).start()

    def take(layer, which):
        @pl.when(me >= 1)
        def _():
            for s in which:
                send(layer, s).wait_recv()

        @pl.when(me < 1)
        def _():
            for s in which:
                halos[layer][s] = jnp.zeros(halos[layer].shape[1:], BF16)

    piece = length // PARTS
    pieces = range(PARTS)

    def ship(slot, s, u, block, where, other):
        rows = pl.ds(u * piece, piece)
        return pltpu.make_async_remote_copy(
            src_ref=block.at[s, rows],
            dst_ref=far.at[where, s, rows],
            send_sem=far_send.at[slot, s, u],
            recv_sem=far_recv.at[where, s, u],
            device_id={"tm": other},
            device_id_type=MESH,
        )

    last_near, last_far = xs.at[near - 1], xs.at[layers - 2]
    relay = (place == 3) & (me >= 7)
    routes = {
        "own": [
            ((place == 3) & (me + 4 < n), 0, last_near, P4, me + 4),
            ((place != 3) & (me + 2 < n), 0, last_near, P2, me + 2),
            ((place == 1) & (me + 3 < n), 1, last_near, P3, me + 3),
            (core == 0, 1, last_near, P1, me + 1),
        ],
        "relay": [
            (relay, 2, far.at[P4], P2, me - 2),
            (relay, 3, far.at[P4], P3, me - 1),
        ],
        "share": [
            ((place == 1) & (me >= 2), 4, far.at[P2], P1, me - 1),
            ((core == 0) & (me >= 2), 4, far.at[P2], P3, me + 1),
        ],
        "early": [(place == 3, 4, far.at[P2], P1, me - 1)],
        "last": [(me + 4 < n, 5, last_far, P9, me + 4)],
    }

    def go(kind, s, which=pieces):
        for ok, slot, block, where, other in routes[kind]:

            @pl.when(ok)
            def _(slot=slot, block=block, where=where, other=other):
                for u in which:
                    ship(slot, s, u, block, where, other).start()

    def get(where, s, least):
        @pl.when(me >= least)
        def _():
            for u in pieces:
                ship(0, s, u, last_near, where, me - 1).wait_recv()

        @pl.when(me < least)
        def _():
            far[where, s] = jnp.zeros(far.shape[2:], BF16)

    def load(layer, s, low, high):
        return source(layer)[s, low:high]

    def stack(parts):
        return jnp.concatenate(parts, axis=0) if len(parts) > 1 else parts[0]

    def gated(layer, late, own_f):
        conv = (taps[layer, 0:1] * late.astype(F32) + taps[layer, 1:2] * own_f).astype(BF16)
        parts = []
        for at in range(0, width, half):
            filt = jnp.dot(conv, wg[layer, 0, :, at : at + half], preferred_element_type=F32)
            gate = jnp.dot(conv, wg[layer, 1, :, at : at + half], preferred_element_type=F32)
            parts.append(tanh_gate(filt, gate))
        return jnp.concatenate(parts, axis=1) if len(parts) > 1 else parts[0]

    def columns():
        return [slice(at, at + half) for at in range(0, width, half)]

    def renewed(layer, z, own_f, cols):
        return (own_f[:, cols] + jnp.dot(z, wr[layer, :, cols], preferred_element_type=F32)).astype(BF16)

    def finish(layer, delayed, own, which, low, high, before=None, between=None):
        count = high - low
        if before:
            before()
        own_f = stack(own).astype(F32)
        z = gated(layer, stack(delayed), own_f)
        for i, s in enumerate(which):
            zs[layer, s, low:high] = z[i * count : (i + 1) * count]
        if between:
            between()
        for cols in columns():
            new = renewed(layer, z, own_f, cols)
            for i, s in enumerate(which):
                xs[layer, s, low:high, cols] = new[i * count : (i + 1) * count]

    top = [max(ALIGN, 2 ** (layer + 1)) for layer in range(clean)]
    first = [0] * clean
    for layer in range(clean - 1, -1, -1):
        need = top[layer] if layer == clean - 1 else first[layer + 1] - 2 ** (layer + 1)
        first[layer] = max(0, min(need, top[layer]) // ALIGN * ALIGN)

    block = min(128, width)
    order = pair_order(block)
    blocks = list(range(width // block))

    def landed(layer):
        for copy in weights(layer)[:2]:
            copy.wait()

    def split(layer, which):
        split_pairs(raw.at[layer], wg.at[layer], order, which)

    def arrive(layer):
        landed(layer)
        split(layer, blocks)

    weights(0)[0].wait()
    split(0, blocks)
    for copy in inputs:
        copy.wait()
    weights(0)[1].wait()
    early, late_blocks = blocks[: len(blocks) // 2], blocks[len(blocks) // 2 :]
    for layer in range(clean):
        delay, low = 2**layer, first[layer]
        landed(layer + 1)
        delayed, own = [], []
        for s in every:
            if delay < ALIGN:
                begin = max(0, low - ALIGN)
                block = pltpu.roll(load(layer, s, begin, length).astype(F32), delay, 0)
                delayed.append(block[low - begin :])
            else:
                delayed.append(load(layer, s, low - delay, length - delay))
            own.append(load(layer, s, low, length))
        finish(
            layer, delayed, own, every, low, length,
            lambda: split(layer + 1, early), lambda: split(layer + 1, late_blocks),
        )
        if layer == 0:
            total = sum(
                ((me + step < n).astype(jnp.int32) + (me >= step).astype(jnp.int32)) for step in range(1, REACH + 1)
            )
            pl.semaphore_wait(barrier, total)
            start_send(0)
        start_send(layer + 1)

    for layer in range(clean):
        delay, high = 2**layer, top[layer]
        take(layer, every)
        delayed, own = [], []
        for s in every:
            rows = rows_of[layer]
            tail = halos[layer][s]
            if delay < ALIGN:
                joined = jnp.concatenate([tail.astype(F32), load(layer, s, 0, high).astype(F32)], axis=0)
                delayed.append(pltpu.roll(joined, delay, 0)[rows:])
            else:
                delayed.append(jnp.concatenate([tail, load(layer, s, 0, high - delay)], axis=0))
            own.append(load(layer, s, 0, high))
        finish(layer, delayed, own, every, 0, high)

    for s in every:
        take(clean, [s])
        late = jnp.concatenate([halos[clean][s], load(clean, s, 0, length - 2**clean)], axis=0)
        finish(clean, [late], [load(clean, s, 0, length)], [s], 0, length)
        go("own", s)

    def early(s):
        for u in pieces:

            @pl.when(place == 3)
            def _(u=u):
                ship(0, s, u, last_near, P2, me - 2).wait_recv()
                ship(4, s, u, far.at[P2], P1, me - 1).start()

            @pl.when(relay)
            def _(u=u):
                ship(0, s, u, last_near, P4, me - 2).wait_recv()

            go("relay", s, [u])

    def share(s):
        for u in pieces:

            @pl.when((place != 3) & (me >= 2))
            def _(u=u):
                ship(0, s, u, last_near, P2, me - 2).wait_recv()

            if u == 0:

                @pl.when(me < 2)
                def _():
                    far[P2, s] = jnp.zeros(far.shape[2:], BF16)

            go("share", s, [u])

    def held_skip(span):
        for cols in columns():
            total = None
            for before in span:
                z = zs[before].reshape(seqs * length, width)
                more = jnp.dot(z, ws[before, :, cols], preferred_element_type=F32)
                total = more if total is None else total + more
            total = total.reshape(seqs, length, half)
            skip[:, :, cols] = total if span[0] == 0 else skip[:, :, cols] + total

    arrive(near)
    arrive(near + 1)
    early(0)
    for layer in range(near + 2, layers):
        arrive(layer)
    for layer in range(layers):
        weights(layer)[2].wait()
    held_skip(range(near // 2))
    early(1)
    held_skip(range(near // 2, near))

    for s in every:
        if 1 < s + 1 < seqs:
            early(s + 1)
        share(s)
        get(P1, s, 1)
        get(P3, s, 3)
        late = jnp.concatenate([far[P1, s], far[P3, s]], axis=0)
        own_f = jnp.concatenate([xs[near - 1, s], far[P2, s]], axis=0).astype(F32)
        z = gated(near, late, own_f)
        zs[near, s] = z[:length]
        for cols in columns():
            new = renewed(near, z, own_f, cols)
            xs[near, s, :, cols] = new[:length]
            ahead[s, :, cols] = new[length:]
        own_f = xs[near, s].astype(F32)
        z = gated(near + 1, ahead[s], own_f)
        zs[near + 1, s] = z
        for cols in columns():
            xs[near + 1, s, :, cols] = renewed(near + 1, z, own_f, cols)
        go("last", s)

    held_skip(range(near, layers - 1))

    final = layers - 1
    for s in every:
        get(P9, s, 4)
        own_f = xs[final - 1, s].astype(F32)
        z = gated(final, far[P9, s], own_f)
        for cols in columns():
            out_x[s, :, cols] = renewed(final, z, own_f, cols)
        for cols in columns():
            more = jnp.dot(z, ws[final, :, cols], preferred_element_type=F32)
            out_skip[s, :, cols] = (skip[s, :, cols] + more).astype(BF16)

    @pl.when(me + 1 < n)
    def _():
        for layer in range(near):
            for s in every:
                send(layer, s).wait_send()

    for route in routes.values():
        for ok, slot, block, where, other in route:

            @pl.when(ok)
            def _(slot=slot, block=block, where=where, other=other):
                for s in every:
                    for u in pieces:
                        ship(slot, s, u, block, where, other).wait_send()


def fused(n, signal, taps, w_gate, w_res, w_skip):
    seqs, length, width = signal.shape
    layers = taps.shape[0]
    near = length.bit_length() - 1
    halos = [pltpu.VMEM((seqs, max(ALIGN, 2**layer), width), BF16) for layer in range(near)]
    flops = 2 * seqs * length * width * width * 4 * layers
    in_vmem, anywhere = pl.BlockSpec(memory_space=pltpu.VMEM), pl.BlockSpec(memory_space=pl.ANY)
    return pl.pallas_call(
        functools.partial(kernel, n, layers, near),
        out_shape=[pltpu.VMEM(signal.shape, BF16)] * 2,
        in_specs=[anywhere] * 5,
        out_specs=[in_vmem, in_vmem],
        scratch_shapes=[
            pltpu.VMEM(signal.shape, BF16),
            pltpu.VMEM(taps.shape, F32),
            pltpu.VMEM((layers, width, 2, width), BF16),
            pltpu.VMEM((layers, 2, width, width), BF16),
            pltpu.VMEM((layers, width, width), BF16),
            pltpu.VMEM((layers, width, width), BF16),
            pltpu.VMEM((layers - 1, seqs, length, width), BF16),
            pltpu.VMEM((layers - 1, seqs, length, width), BF16),
            pltpu.VMEM((seqs, length, width), F32),
            pltpu.VMEM((seqs, length, width), BF16),
            pltpu.VMEM((5, seqs, length, width), BF16),
            pltpu.SemaphoreType.DMA((2,)),
            pltpu.SemaphoreType.DMA((layers, 3)),
            pltpu.SemaphoreType.DMA((near, seqs)),
            pltpu.SemaphoreType.DMA((near, seqs)),
            pltpu.SemaphoreType.DMA((6, seqs, PARTS)),
            pltpu.SemaphoreType.DMA((5, seqs, PARTS)),
            pltpu.SemaphoreType.REGULAR,
            *halos,
        ],
        compiler_params=pltpu.CompilerParams(collective_id=0, has_side_effects=True, vmem_limit_bytes=VMEM_LIMIT),
        cost_estimate=pl.CostEstimate(flops=flops, bytes_accessed=8 * layers * width * width, transcendentals=0),
        name="stack",
    )(signal, taps, w_gate, w_res, w_skip)


def solution(mesh):
    in_specs = (
        P(None, "tm", "chan"),
        P(None, None, "chan"),
        P(None, None, None, "chan"),
        P(None, None, "chan"),
        P(None, None, "chan"),
    )
    out_specs = (P(None, "tm", "chan"), P(None, "tm", "chan"))

    def body(*args):
        n, length, layers = mesh.shape["tm"], args[0].shape[1], args[1].shape[0]
        fits = length >= 4 * ALIGN and 2 ** (layers - 3) == length and n % 4 == 0
        if mesh.shape["chan"] == 1 and fits:
            return tuple(fused(n, *args))
        return local(*args)

    return jax.shard_map(body, mesh=mesh, in_specs=in_specs, out_specs=out_specs, check_vma=False)
```

```python
import functools

import jax
import jax.numpy as jnp
from jax import lax
from jax.experimental import pallas as pl
from jax.experimental.pallas import tpu as pltpu
from jax.sharding import PartitionSpec as P

MESH = pl.DeviceIdType.MESH
BF16, F32 = jnp.bfloat16, jnp.float32
ALIGN = 16
VMEM_LIMIT = 56000 * 1024


def shifted(value, axis, steps):
    count = lax.axis_size(axis)
    leading, last = (max(0, -steps), min(count, count - steps))
    return lax.ppermute(value, axis, [(source, source + steps) for source in range(leading, last)])


def delay_block(stream, delay, near_fn, far_fn):
    length = stream.shape[1]
    whole, rest = divmod(delay, length)
    if whole == 0:
        nearer = stream
    else:
        nearer = near_fn(stream, whole)
    if rest == 0:
        return nearer
    farther = far_fn(stream[:, length - rest :], whole + 1)
    return jnp.concatenate([farther, nearer[:, : length - rest]], axis=1)


def near_time(block, steps):
    return shifted(block, "tm", steps)


def far_time(block, steps):
    return shifted(block, "tm", steps)


def gate_units(hidden):
    return (jnp.tanh(hidden[:, :, 0]) * jax.nn.sigmoid(hidden[:, :, 1])).astype(jnp.bfloat16)


def local(signal, taps, w_gate, w_res, w_skip):
    stream = signal
    seqs, length, local_c = stream.shape
    skip = jnp.zeros((seqs, length, local_c), jnp.float32)
    for layer in range(taps.shape[0]):
        delayed = delay_block(stream, 2**layer, near_time, far_time)
        conv = (
            taps[layer, 0] * delayed.astype(jnp.float32)
            + taps[layer, 1] * stream.astype(jnp.float32)
        ).astype(jnp.bfloat16)
        gate_w = w_gate[layer]
        hidden = jnp.einsum(
            "stc,cko->stko",
            lax.all_gather(conv, "chan", axis=2, tiled=True),
            gate_w,
            preferred_element_type=jnp.float32,
        )
        gated = gate_units(hidden)
        res_w = w_res[layer]
        skip_w = w_skip[layer]
        piece = lax.all_gather(gated, "chan", axis=2, tiled=True)
        update = jnp.einsum("stc,co->sto", piece, res_w, preferred_element_type=jnp.float32)
        skip_part = jnp.einsum("stc,co->sto", piece, skip_w, preferred_element_type=jnp.float32)
        stream = (stream.astype(jnp.float32) + update).astype(jnp.bfloat16)
        skip = skip + skip_part
    return (stream, skip.astype(jnp.bfloat16))


def tanh_gate(filt, gate):
    return (jnp.tanh(filt) * (0.5 * jnp.tanh(0.5 * gate) + 0.5)).astype(BF16)


def pair_order(block):
    row = lax.broadcasted_iota(jnp.int32, (2 * block, 2 * block), 0)
    column = lax.broadcasted_iota(jnp.int32, (2 * block, 2 * block), 1)
    wanted = jnp.where(row < block, 2 * row, 2 * (row - block) + 1)
    return jnp.where(column == wanted, 1.0, 0.0).astype(F32).astype(BF16)


def split_pairs(pairs, out, order, blocks):
    block = order.shape[0] // 2
    for index in blocks:
        at = index * block
        both = pairs[at : at + block].reshape(2 * block, pairs.shape[2])
        sorted_rows = jnp.dot(order, both, preferred_element_type=F32).astype(BF16)
        out[0, at : at + block] = sorted_rows[:block]
        out[1, at : at + block] = sorted_rows[block:]


P1, P2, P3, P4, P9 = range(5)
REACH = 4
PARTS = 2


def kernel(n, layers, near, sig_hbm, taps_hbm, wg_hbm, wr_hbm, ws_hbm, out_x, out_skip, *scratch):
    sig, taps, raw, wg, wr, ws, xs, zs, skip, ahead, far = scratch[:11]
    in_sem, w_sem, send_sem, recv_sem, far_send, far_recv, order_sem = scratch[11:18]
    halos = scratch[18:]
    seqs, length, width = sig.shape
    me = lax.axis_index("tm")
    place = lax.rem(me, 4)
    core = lax.rem(me, 2)
    clean = near - 1
    rows_of = [max(ALIGN, 2**layer) for layer in range(near)]
    half = min(256, width)
    every = list(range(seqs))

    def fence():
        pl.semaphore_signal(order_sem, 1)
        pl.semaphore_wait(order_sem, 1)

    def weights(layer):
        return [
            pltpu.make_async_copy(wg_hbm.at[layer], raw.at[layer], w_sem.at[layer, 0]),
            pltpu.make_async_copy(wr_hbm.at[layer], wr.at[layer], w_sem.at[layer, 1]),
            pltpu.make_async_copy(ws_hbm.at[layer], ws.at[layer], w_sem.at[layer, 2]),
        ]

    inputs = [
        pltpu.make_async_copy(sig_hbm, sig, in_sem.at[0]),
        pltpu.make_async_copy(taps_hbm, taps, in_sem.at[1]),
    ]
    weights(0)[0].start()
    fence()
    for copy in inputs:
        copy.start()
    fence()
    weights(0)[1].start()
    fence()
    for layer in range(1, layers):
        for copy in weights(layer)[:2]:
            copy.start()
        if layer <= near:
            fence()
    fence()
    for layer in range(layers):
        weights(layer)[2].start()

    barrier = pltpu.get_barrier_semaphore()
    for step in range(1, REACH + 1):
        for ok, other in ((me + step < n, me + step), (me >= step, me - step)):

            @pl.when(ok)
            def _(other=other):
                pl.semaphore_signal(barrier, inc=1, device_id={"tm": other}, device_id_type=MESH)

    def source(layer):
        return sig if layer == 0 else xs.at[layer - 1]

    def send(layer, s):
        rows = rows_of[layer]
        return pltpu.make_async_remote_copy(
            src_ref=source(layer).at[s, pl.ds(length - rows, rows)],
            dst_ref=halos[layer].at[s],
            send_sem=send_sem.at[layer, s],
            recv_sem=recv_sem.at[layer, s],
            device_id={"tm": me + 1},
            device_id_type=MESH,
        )

    def start_send(layer):
        @pl.when(me + 1 < n)
        def _():
            for s in every:
                send(layer, s).start()

    def take(layer, which):
        @pl.when(me >= 1)
        def _():
            for s in which:
                send(layer, s).wait_recv()

        @pl.when(me < 1)
        def _():
            for s in which:
                halos[layer][s] = jnp.zeros(halos[layer].shape[1:], BF16)

    piece = length // PARTS
    pieces = range(PARTS)

    def ship(slot, s, u, block, where, other):
        rows = pl.ds(u * piece, piece)
        return pltpu.make_async_remote_copy(
            src_ref=block.at[s, rows],
            dst_ref=far.at[where, s, rows],
            send_sem=far_send.at[slot, s, u],
            recv_sem=far_recv.at[where, s, u],
            device_id={"tm": other},
            device_id_type=MESH,
        )

    last_near, last_far = xs.at[near - 1], xs.at[layers - 2]
    relay = (place == 3) & (me >= 7)
    routes = {
        "own": [
            ((place == 3) & (me + 4 < n), 0, last_near, P4, me + 4),
            (core == 0, 1, last_near, P1, me + 1),
        ],
        "next": [
            ((place != 3) & (me + 2 < n), 0, last_near, P2, me + 2),
            ((place == 1) & (me + 3 < n), 1, last_near, P3, me + 3),
        ],
        "relay": [
            (relay, 2, far.at[P4], P2, me - 2),
            (relay, 3, far.at[P4], P3, me - 1),
        ],
        "share": [
            ((place == 1) & (me >= 2), 4, far.at[P2], P1, me - 1),
            ((core == 0) & (me >= 2), 4, far.at[P2], P3, me + 1),
        ],
        "early": [(place == 3, 4, far.at[P2], P1, me - 1)],
        "last": [(me + 4 < n, 5, last_far, P9, me + 4)],
    }

    def go(kind, s, which=pieces):
        for ok, slot, block, where, other in routes[kind]:

            @pl.when(ok)
            def _(slot=slot, block=block, where=where, other=other):
                for u in which:
                    ship(slot, s, u, block, where, other).start()

    def get(where, s, least):
        @pl.when(me >= least)
        def _():
            for u in pieces:
                ship(0, s, u, last_near, where, me - 1).wait_recv()

        @pl.when(me < least)
        def _():
            far[where, s] = jnp.zeros(far.shape[2:], BF16)

    def load(layer, s, low, high):
        return source(layer)[s, low:high]

    def stack(parts):
        return jnp.concatenate(parts, axis=0) if len(parts) > 1 else parts[0]

    def gated(layer, late, own_f):
        conv = (taps[layer, 0:1] * late.astype(F32) + taps[layer, 1:2] * own_f).astype(BF16)
        parts = []
        for at in range(0, width, half):
            filt = jnp.dot(conv, wg[layer, 0, :, at : at + half], preferred_element_type=F32)
            gate = jnp.dot(conv, wg[layer, 1, :, at : at + half], preferred_element_type=F32)
            parts.append(tanh_gate(filt, gate))
        return jnp.concatenate(parts, axis=1) if len(parts) > 1 else parts[0]

    def columns():
        return [slice(at, at + half) for at in range(0, width, half)]

    def renewed(layer, z, own_f, cols):
        return (own_f[:, cols] + jnp.dot(z, wr[layer, :, cols], preferred_element_type=F32)).astype(BF16)

    def finish(layer, delayed, own, which, low, high, before=None, between=None):
        count = high - low
        if before:
            before()
        own_f = stack(own).astype(F32)
        z = gated(layer, stack(delayed), own_f)
        for i, s in enumerate(which):
            zs[layer, s, low:high] = z[i * count : (i + 1) * count]
        if between:
            between()
        for cols in columns():
            new = renewed(layer, z, own_f, cols)
            for i, s in enumerate(which):
                xs[layer, s, low:high, cols] = new[i * count : (i + 1) * count]

    top = [max(ALIGN, 2 ** (layer + 1)) for layer in range(clean)]
    first = [0] * clean
    for layer in range(clean - 1, -1, -1):
        need = top[layer] if layer == clean - 1 else first[layer + 1] - 2 ** (layer + 1)
        first[layer] = max(0, min(need, top[layer]) // ALIGN * ALIGN)

    block = min(128, width)
    order = pair_order(block)
    blocks = list(range(width // block))

    def landed(layer):
        for copy in weights(layer)[:2]:
            copy.wait()

    def split(layer, which):
        split_pairs(raw.at[layer], wg.at[layer], order, which)

    def arrive(layer):
        landed(layer)
        split(layer, blocks)

    weights(0)[0].wait()
    split(0, blocks)
    for copy in inputs:
        copy.wait()
    weights(0)[1].wait()
    early, late_blocks = blocks[: len(blocks) // 2], blocks[len(blocks) // 2 :]
    for layer in range(clean):
        delay, low = 2**layer, first[layer]
        landed(layer + 1)
        delayed, own = [], []
        for s in every:
            if delay < ALIGN:
                begin = max(0, low - ALIGN)
                block = pltpu.roll(load(layer, s, begin, length).astype(F32), delay, 0)
                delayed.append(block[low - begin :])
            else:
                delayed.append(load(layer, s, low - delay, length - delay))
            own.append(load(layer, s, low, length))
        finish(
            layer, delayed, own, every, low, length,
            lambda: split(layer + 1, early), lambda: split(layer + 1, late_blocks),
        )
        if layer == 0:
            total = sum(
                ((me + step < n).astype(jnp.int32) + (me >= step).astype(jnp.int32)) for step in range(1, REACH + 1)
            )
            pl.semaphore_wait(barrier, total)
            start_send(0)
        start_send(layer + 1)

    for layer in range(clean):
        delay, high = 2**layer, top[layer]
        take(layer, every)
        delayed, own = [], []
        for s in every:
            rows = rows_of[layer]
            tail = halos[layer][s]
            if delay < ALIGN:
                joined = jnp.concatenate([tail.astype(F32), load(layer, s, 0, high).astype(F32)], axis=0)
                delayed.append(pltpu.roll(joined, delay, 0)[rows:])
            else:
                delayed.append(jnp.concatenate([tail, load(layer, s, 0, high - delay)], axis=0))
            own.append(load(layer, s, 0, high))
        finish(layer, delayed, own, every, 0, high)

    for s in every:
        take(clean, [s])
        late = jnp.concatenate([halos[clean][s], load(clean, s, 0, length - 2**clean)], axis=0)
        finish(clean, [late], [load(clean, s, 0, length)], [s], 0, length)
        go("own", s)
        if s == 0:
            go("next", s)

    def early(s):
        for u in pieces:

            @pl.when(place == 3)
            def _(u=u):
                ship(0, s, u, last_near, P2, me - 2).wait_recv()
                ship(4, s, u, far.at[P2], P1, me - 1).start()

            @pl.when(relay)
            def _(u=u):
                ship(0, s, u, last_near, P4, me - 2).wait_recv()

            go("relay", s, [u])

    def share(s):
        for u in pieces:

            @pl.when((place != 3) & (me >= 2))
            def _(u=u):
                ship(0, s, u, last_near, P2, me - 2).wait_recv()

            if u == 0:

                @pl.when(me < 2)
                def _():
                    far[P2, s] = jnp.zeros(far.shape[2:], BF16)

            go("share", s, [u])

    def held_skip(span):
        for cols in columns():
            total = None
            for before in span:
                z = zs[before].reshape(seqs * length, width)
                more = jnp.dot(z, ws[before, :, cols], preferred_element_type=F32)
                total = more if total is None else total + more
            total = total.reshape(seqs, length, half)
            skip[:, :, cols] = total if span[0] == 0 else skip[:, :, cols] + total

    arrive(near)
    for s in every[1:2]:
        go("next", s)
    arrive(near + 1)
    early(0)
    for s in every[2:]:
        go("next", s)
    for layer in range(near + 2, layers):
        arrive(layer)
    for layer in range(layers):
        weights(layer)[2].wait()
    held_skip(range(near // 2))
    early(1)
    held_skip(range(near // 2, near))

    for s in every:
        if 1 < s + 1 < seqs:
            early(s + 1)
        share(s)
        get(P1, s, 1)
        get(P3, s, 3)
        late = jnp.concatenate([far[P1, s], far[P3, s]], axis=0)
        own_f = jnp.concatenate([xs[near - 1, s], far[P2, s]], axis=0).astype(F32)
        z = gated(near, late, own_f)
        zs[near, s] = z[:length]
        for cols in columns():
            new = renewed(near, z, own_f, cols)
            xs[near, s, :, cols] = new[:length]
            ahead[s, :, cols] = new[length:]
        own_f = xs[near, s].astype(F32)
        z = gated(near + 1, ahead[s], own_f)
        zs[near + 1, s] = z
        for cols in columns():
            xs[near + 1, s, :, cols] = renewed(near + 1, z, own_f, cols)
        go("last", s)

    held_skip(range(near, layers - 1))

    final = layers - 1
    for s in every:
        get(P9, s, 4)
        own_f = xs[final - 1, s].astype(F32)
        z = gated(final, far[P9, s], own_f)
        for cols in columns():
            out_x[s, :, cols] = renewed(final, z, own_f, cols)
        for cols in columns():
            more = jnp.dot(z, ws[final, :, cols], preferred_element_type=F32)
            out_skip[s, :, cols] = (skip[s, :, cols] + more).astype(BF16)

    @pl.when(me + 1 < n)
    def _():
        for layer in range(near):
            for s in every:
                send(layer, s).wait_send()

    for route in routes.values():
        for ok, slot, block, where, other in route:

            @pl.when(ok)
            def _(slot=slot, block=block, where=where, other=other):
                for s in every:
                    for u in pieces:
                        ship(slot, s, u, block, where, other).wait_send()


def fused(n, signal, taps, w_gate, w_res, w_skip):
    seqs, length, width = signal.shape
    layers = taps.shape[0]
    near = length.bit_length() - 1
    halos = [pltpu.VMEM((seqs, max(ALIGN, 2**layer), width), BF16) for layer in range(near)]
    flops = 2 * seqs * length * width * width * 4 * layers
    in_vmem, anywhere = pl.BlockSpec(memory_space=pltpu.VMEM), pl.BlockSpec(memory_space=pl.ANY)
    return pl.pallas_call(
        functools.partial(kernel, n, layers, near),
        out_shape=[pltpu.VMEM(signal.shape, BF16)] * 2,
        in_specs=[anywhere] * 5,
        out_specs=[in_vmem, in_vmem],
        scratch_shapes=[
            pltpu.VMEM(signal.shape, BF16),
            pltpu.VMEM(taps.shape, F32),
            pltpu.VMEM((layers, width, 2, width), BF16),
            pltpu.VMEM((layers, 2, width, width), BF16),
            pltpu.VMEM((layers, width, width), BF16),
            pltpu.VMEM((layers, width, width), BF16),
            pltpu.VMEM((layers - 1, seqs, length, width), BF16),
            pltpu.VMEM((layers - 1, seqs, length, width), BF16),
            pltpu.VMEM((seqs, length, width), F32),
            pltpu.VMEM((seqs, length, width), BF16),
            pltpu.VMEM((5, seqs, length, width), BF16),
            pltpu.SemaphoreType.DMA((2,)),
            pltpu.SemaphoreType.DMA((layers, 3)),
            pltpu.SemaphoreType.DMA((near, seqs)),
            pltpu.SemaphoreType.DMA((near, seqs)),
            pltpu.SemaphoreType.DMA((6, seqs, PARTS)),
            pltpu.SemaphoreType.DMA((5, seqs, PARTS)),
            pltpu.SemaphoreType.REGULAR,
            *halos,
        ],
        compiler_params=pltpu.CompilerParams(collective_id=0, has_side_effects=True, vmem_limit_bytes=VMEM_LIMIT),
        cost_estimate=pl.CostEstimate(flops=flops, bytes_accessed=8 * layers * width * width, transcendentals=0),
        name="stack",
    )(signal, taps, w_gate, w_res, w_skip)


def solution(mesh):
    in_specs = (
        P(None, "tm", "chan"),
        P(None, None, "chan"),
        P(None, None, None, "chan"),
        P(None, None, "chan"),
        P(None, None, "chan"),
    )
    out_specs = (P(None, "tm", "chan"), P(None, "tm", "chan"))

    def body(*args):
        n, length, layers = mesh.shape["tm"], args[0].shape[1], args[1].shape[0]
        fits = length >= 4 * ALIGN and 2 ** (layers - 3) == length and n % 4 == 0
        if mesh.shape["chan"] == 1 and fits:
            return tuple(fused(n, *args))
        return local(*args)

    return jax.shard_map(body, mesh=mesh, in_specs=in_specs, out_specs=out_specs, check_vma=False)
```
